64 devices in a mesh: data: 4 (over x, y), sp: 16 (over z, core).
Axes of the slice: x: 2, y: 2, z: 8, core: 2. Of those that a mesh axis runs over, the one named last changes fastest.
The devices are a block of a 4x4x8 slice.
Arguments:
- latents: bfloat16 [8, 32, 512, 1152], P('data', 'sp'), parts along dimension 0
- valid_len: int32 [8], P('data'), parts along dimension 0
- norm_w: bfloat16 [2, 4, 1152], replicated
- w_qkv: bfloat16 [2, 1152, 3456], replicated
- w_out: bfloat16 [2, 16, 72, 1152], replicated
- w_up: bfloat16 [2, 1152, 4608], replicated
- w_down: bfloat16 [2, 4608, 1152], replicated
Outputs:
- output: bfloat16 [8, 32, 512, 1152], P('data', 'sp'), parts along dimension 0
There are 4 independent parts. The reference program is written for one: setup_inputs(seed, part) draws one part's arguments, and reference() takes and returns one part's arrays. A program takes and returns all parts, laid end to end along the dimension named above; an argument that names none is the same for every part.
All inputs are finite; a program needn't handle non-finite values.
Results may differ from the reference program's by a relative error of at most 0.0158405.
Values are sent between devices in bfloat16 or wider.
A program may use at most 768 MiB of HBM per device.

```python
import jax
import jax.numpy as jnp
from jax import lax

D = 1152
HEADS = 16
BATCH = 2
FRAMES = 32
PATCHES = 512

HEAD_DIM = D // HEADS
LN_EPS = 1e-6
NEG_BIG = -1e30


def setup_inputs(seed: int = 0, part: int = 0) -> dict:
    part_key = jax.random.fold_in(jax.random.key(seed), part)
    lat_keys = jax.random.split(part_key, 4)
    token_noise = jax.random.normal(lat_keys[0], (BATCH, FRAMES, PATCHES, D), jnp.float32)
    frame_term = jax.random.normal(lat_keys[1], (BATCH, FRAMES, 1, D), jnp.float32)
    patch_term = jax.random.normal(lat_keys[2], (BATCH, 1, PATCHES, D), jnp.float32)
    latents = (token_noise + 0.8 * frame_term + 0.8 * patch_term).astype(jnp.bfloat16)
    len_keys = jax.random.split(lat_keys[3], 2)
    drawn_len = jax.random.randint(len_keys[0], (BATCH,), 1, FRAMES + 1)
    full_video = jax.random.randint(len_keys[1], (), 0, BATCH)
    valid_len = jnp.where(jnp.arange(BATCH) == full_video, FRAMES, drawn_len).astype(jnp.int32)
    weight_keys = jax.random.split(jax.random.key(seed + 1), 6)
    ln_gains = 1.0 + 0.2 * jax.random.normal(weight_keys[0], (2, 2, D), jnp.float32)
    ln_shifts = 0.2 * jax.random.normal(weight_keys[1], (2, 2, D), jnp.float32)
    norm_w = jnp.stack([ln_gains[:, 0], ln_shifts[:, 0], ln_gains[:, 1], ln_shifts[:, 1]], axis=1).astype(jnp.bfloat16)
    col_scale = jnp.concatenate([jnp.full((2 * D,), 1.5, jnp.float32), jnp.ones((D,), jnp.float32)])
    w_qkv = (jax.random.normal(weight_keys[2], (2, D, 3 * D), jnp.float32) * (col_scale * D ** -0.5)).astype(jnp.bfloat16)
    w_out = (jax.random.normal(weight_keys[3], (2, HEADS, HEAD_DIM, D), jnp.float32) * D ** -0.5).astype(jnp.bfloat16)
    w_up = (jax.random.normal(weight_keys[4], (2, D, 4 * D), jnp.float32) * D ** -0.5).astype(jnp.bfloat16)
    w_down = (jax.random.normal(weight_keys[5], (2, 4 * D, D), jnp.float32) * (4 * D) ** -0.5).astype(jnp.bfloat16)
    return {'latents': latents, 'valid_len': valid_len, 'norm_w': norm_w, 'w_qkv': w_qkv, 'w_out': w_out, 'w_up': w_up, 'w_down': w_down}


def layer_norm(tokens, ln_gain, ln_shift):
    values = tokens.astype(jnp.float32)
    average = jnp.mean(values, axis=-1, keepdims=True)
    centered = values - average
    variance = jnp.mean(centered * centered, axis=-1, keepdims=True)
    normed = centered * lax.rsqrt(variance + LN_EPS)
    return (normed * ln_gain.astype(jnp.float32) + ln_shift.astype(jnp.float32)).astype(jnp.bfloat16)


def project(tokens, weight):
    flat_rows = tokens.reshape(-1, tokens.shape[-1])
    result = jnp.dot(flat_rows, weight, preferred_element_type=jnp.float32).astype(jnp.bfloat16)
    return result.reshape(tokens.shape[:-1] + (weight.shape[-1],))


def residual(base_act, delta_act):
    return (base_act.astype(jnp.float32) + delta_act.astype(jnp.float32)).astype(jnp.bfloat16)


def attend_one(qkv_seq, allowed):
    seq_len = qkv_seq.shape[0]
    query_h = qkv_seq[:, :D].reshape(seq_len, HEADS, HEAD_DIM).astype(jnp.float32)
    key_h = qkv_seq[:, D:2 * D].reshape(seq_len, HEADS, HEAD_DIM).astype(jnp.float32)
    value_h = qkv_seq[:, 2 * D:].reshape(seq_len, HEADS, HEAD_DIM).astype(jnp.float32)
    scores = jnp.einsum('qhd,khd->hqk', query_h, key_h) * HEAD_DIM ** -0.5
    if allowed is not None:
        scores = jnp.where(allowed[None], scores, NEG_BIG)
    attn_prob = jax.nn.softmax(scores, axis=-1).astype(jnp.bfloat16).astype(jnp.float32)
    attn_out = jnp.einsum('hqk,khd->qhd', attn_prob, value_h)
    return attn_out.astype(jnp.bfloat16).reshape(seq_len, D)


def dit_block(tokens, layer_idx, params, attend_all):
    norm_w, w_qkv, w_out, w_up, w_down = params
    normed = layer_norm(tokens, norm_w[layer_idx, 0], norm_w[layer_idx, 1])
    attn_out = attend_all(project(normed, w_qkv[layer_idx]))
    hidden = residual(tokens, project(attn_out, w_out[layer_idx].reshape(D, D)))
    normed_mlp = layer_norm(hidden, norm_w[layer_idx, 2], norm_w[layer_idx, 3])
    gelu_act = jax.nn.gelu(project(normed_mlp, w_up[layer_idx]).astype(jnp.float32), approximate=True).astype(jnp.bfloat16)
    return residual(hidden, project(gelu_act, w_down[layer_idx]))


def video_forward(video_lat, length, params):
    frame_pos = jnp.arange(FRAMES)
    causal = (frame_pos[None, :] <= frame_pos[:, None]) & (frame_pos[None, :] < length)

    def spatial_attend(qkv_proj):
        def one_frame(frame_qkv):
            return attend_one(frame_qkv, None)
        return lax.map(one_frame, qkv_proj)

    def temporal_attend(qkv_proj):
        def one_patch(patch_qkv):
            return attend_one(patch_qkv, causal)
        return jnp.swapaxes(lax.map(one_patch, jnp.swapaxes(qkv_proj, 0, 1)), 0, 1)

    spatial = dit_block(video_lat, 0, params, spatial_attend)
    return dit_block(spatial, 1, params, temporal_attend)


def reference(latents, valid_len, norm_w, w_qkv, w_out, w_up, w_down):
    params = (norm_w, w_qkv, w_out, w_up, w_down)

    def one_video(video_item):
        return video_forward(video_item[0], video_item[1], params)
    return lax.map(one_video, (latents, valid_len))
```

```python
import functools
import math

import jax
import jax.numpy as jnp
from jax import lax
from jax.experimental import pallas as pl
from jax.experimental.pallas import tpu as pltpu
from jax.sharding import PartitionSpec as P

LN_EPS = 1e-6
MASKED = -1e30
OPEN = 3e38
LANES = 128
f32, bf16 = jnp.float32, jnp.bfloat16
MESH = pl.DeviceIdType.MESH


def layer_norm(tokens, gain, shift):
    values = tokens.astype(f32)
    inv_width = 1.0 / values.shape[-1]
    centered = values - jnp.sum(values, -1, keepdims=True) * inv_width
    variance = jnp.sum(centered * centered, -1, keepdims=True) * inv_width
    return (centered * lax.rsqrt(variance + LN_EPS) * gain + shift).astype(bf16)


def project(a, b):
    return jnp.dot(a, b, preferred_element_type=f32).astype(bf16)


def residual(base, delta):
    return (base.astype(f32) + delta.astype(f32)).astype(bf16)


def gelu(u):
    x = u.astype(f32)
    c = math.sqrt(2.0 / math.pi)
    half = 0.5 * x
    return (half + half * jnp.tanh(x * (x * x * (c * 0.044715) + c))).astype(bf16)


def head_windows(heads, head_dim):
    out = []
    for h in range(heads):
        lo = h * head_dim
        base = lo // LANES * LANES
        out.append((lo, base, LANES if lo + head_dim <= base + LANES else 2 * LANES))
    return out


def attention(qkv, a_ref, cap_ref, heads, head_dim):
    width = heads * head_dim
    scale = head_dim ** -0.5 * math.log2(math.e)
    wins = head_windows(heads, head_dim)

    def lanes(h):
        _, base, w = wins[h]
        return lax.broadcasted_iota(jnp.int32, (1, w), 1) + base

    def scores(h):
        lo, base, w = wins[h]
        lane = lanes(h)
        own = jnp.where((lane >= lo) & (lane < lo + head_dim), 1.0, 0.0).astype(bf16)
        q = qkv[:, base:base + w] * own
        k = qkv[:, width + base:width + base + w]
        return lax.dot_general(q, k, (((1,), (1,)), ((), ())), preferred_element_type=f32)

    ahead = scores(0)
    for h in range(heads):
        s, ahead = ahead, scores(h + 1) if h + 1 < heads else None
        lo, base, w = wins[h]
        s = jnp.minimum(s * scale, cap_ref[...])
        e = jnp.exp2(s - jnp.max(s, -1, keepdims=True))
        p = (e * (1.0 / jnp.sum(e, -1, keepdims=True))).astype(bf16)
        o = project(p, qkv[:, 2 * width + base:2 * width + base + w])
        if lo != base:
            o = jnp.where(jnp.broadcast_to(lanes(h) >= lo, o.shape), o, a_ref[:, base:base + w])
        a_ref[:, base:base + w] = o


def kernel(n_sp, heads, head_dim, x_hbm, len_ref, norm_ref, wqkv_hbm, wout_hbm, wup_hbm, wdown_hbm, y_hbm,
           wqkv, wout, wup, wdown, xb, qkv, ab, hb, nb, ub, zb, rb, cap,
           w_sem, x_sem, send_sem, recv_sem, y_sem, own_sem):
    videos, frames, rows, width = x_hbm.shape
    steps = videos * frames
    per_dev = rows // n_sp
    per_chunk = rows // (n_sp * frames)
    chunks = per_dev // per_chunk
    half = rows // 2
    me = lax.axis_index("sp")
    peers = n_sp - 1

    barrier = pltpu.get_barrier_semaphore()

    @pl.loop(1, n_sp)
    def _(k):
        pl.semaphore_signal(barrier, inc=1, device_id={"sp": lax.rem(me + k, n_sp)}, device_id_type=MESH)

    weights = ((wqkv_hbm, wqkv), (wout_hbm, wout), (wup_hbm, wup), (wdown_hbm, wdown))

    def load(i, layer):
        return pltpu.make_async_copy(weights[i][0].at[layer], weights[i][1], w_sem.at[i])

    def load_x(s):
        return pltpu.make_async_copy(x_hbm.at[s // frames, s % frames], xb.at[s % 2], x_sem.at[s % 2])

    load_x(0).start()
    for i in range(4):
        load(i, 0).start()
    cap[...] = jnp.full(cap.shape, OPEN, f32)
    pl.semaphore_wait(barrier, peers)

    def send(s, j):
        t = me * frames + s % frames
        return pltpu.make_async_remote_copy(
            src_ref=zb.at[s, pl.ds(j * per_dev, per_dev), :], dst_ref=rb.at[s // frames, t],
            send_sem=send_sem.at[s], recv_sem=recv_sem.at[s // frames], device_id={"sp": j}, device_id_type=MESH)

    def give(c, j, f):
        v, part = c // chunks, c % chunks
        return pltpu.make_async_remote_copy(
            src_ref=zb.at[c, pl.ds((j * frames + f) * per_chunk, per_chunk), :],
            dst_ref=y_hbm.at[v, f, pl.ds(me * per_dev + part * per_chunk, per_chunk), :],
            send_sem=send_sem.at[c], recv_sem=y_sem, device_id={"sp": j}, device_id_type=MESH)

    def keep(c, f):
        v, part = c // chunks, c % chunks
        return pltpu.make_async_copy(
            zb.at[c, pl.ds((me * frames + f) * per_chunk, per_chunk), :],
            y_hbm.at[v, f, pl.ds(me * per_dev + part * per_chunk, per_chunk), :], own_sem)

    def wait_sent(slot):
        sent = zb.at[slot, pl.ds(0, peers * per_dev), :]
        pltpu.make_async_copy(sent, sent, send_sem.at[slot]).wait()

    @pl.loop(0, 2 * steps)
    def _(s):
        spatial = s < steps
        layer = s // steps
        slot = s % steps
        c = s - steps
        xs = xb.at[s % 2]

        @pl.when(spatial)
        def _():
            load_x(s).wait()

        @pl.when(s + 1 < steps)
        def _():
            load_x(s + 1).start()

        @pl.when(jnp.logical_and(s >= steps, slot % chunks == 0))
        def _():
            v = slot // chunks
            got = rb.at[v, pl.ds(0, peers * frames)]
            pltpu.make_async_copy(got, got, recv_sem.at[v]).wait()
            shift = per_chunk.bit_length() - 1
            limit = len_ref[v]
            for r in range(0, rows, LANES):
                qi = lax.broadcasted_iota(jnp.int32, (LANES, rows), 0) + r
                ki = lax.broadcasted_iota(jnp.int32, (LANES, rows), 1)
                kt = lax.shift_right_logical(ki, shift)
                ok = ((qi & (per_chunk - 1)) == (ki & (per_chunk - 1))) & (kt <= lax.shift_right_logical(qi, shift)) & (kt < limit)
                cap[r:r + LANES, :] = jnp.where(ok, OPEN, MASKED)

        @pl.when(s >= steps)
        def _():
            part = slot % chunks
            piece = rb[slot // chunks, :, pl.ds(part * per_chunk, per_chunk), :]
            xs[...] = piece.reshape(rows, width)

        norms = norm_ref[layer].astype(f32)
        for r in range(0, rows, half):
            nb[r:r + half, :] = layer_norm(xs[r:r + half, :], norms[0:1], norms[1:2])

        @pl.when(slot == 0)
        def _():
            load(0, layer).wait()

        qkv[...] = project(nb[...], wqkv[...])

        @pl.when(s == steps - 1)
        def _():
            load(0, 1).start()

        attention(qkv, ab, cap, heads, head_dim)

        @pl.when(slot == 0)
        def _():
            for i in range(1, 4):
                load(i, layer).wait()

        @pl.when(s >= steps)
        def _():
            wait_sent(slot)

        @pl.loop(0, 2)
        def _(m):
            at = pl.ds(pl.multiple_of(m * half, half), half)
            norms = norm_ref[layer].astype(f32)
            hb[...] = residual(xs[at, :], project(ab[at, :], wout[...]))
            nb[at, :] = layer_norm(hb[...], norms[2:3], norms[3:4])
            ub[...] = gelu(project(nb[at, :], wup[...]))
            zb[slot, at, :] = residual(hb[...], project(ub[...], wdown[...]))

        @pl.when(s == steps - 1)
        def _():
            for i in range(1, 4):
                load(i, 1).start()

        @pl.when(spatial)
        def _():
            @pl.loop(1, n_sp)
            def _(k):
                send(s, lax.rem(me + k, n_sp)).start()
            rb[s // frames, me * frames + s % frames] = zb[s, pl.ds(pl.multiple_of(me * per_dev, per_dev), per_dev), :]

        @pl.when(s >= steps)
        def _():
            @pl.loop(1, n_sp)
            def _(k):
                for f in range(frames):
                    give(c, lax.rem(me + k, n_sp), f).start()
            for f in range(frames):
                keep(c, f).start()

    for slot in range(steps):
        wait_sent(slot)
    kept = y_hbm.at[:, :, pl.ds(0, per_dev), :]
    pltpu.make_async_copy(kept, kept, own_sem).wait()
    got = y_hbm.at[:, :, pl.ds(0, peers * per_dev), :]
    pltpu.make_async_copy(got, got, y_sem).wait()


def solution(mesh):
    act_spec = P('data', 'sp', None, None)
    n_sp = mesh.shape['sp']

    def local_step(latents, valid_len, norm_w, w_qkv, w_out, w_up, w_down):
        videos, frames, rows, width = latents.shape
        heads, head_dim = w_out.shape[1:3]
        hidden = w_up.shape[2]
        tokens = videos * frames * rows
        half = rows // 2
        any_spec = pl.BlockSpec(memory_space=pl.ANY)
        dma = pltpu.SemaphoreType.DMA
        steps = videos * frames
        return pl.pallas_call(
            functools.partial(kernel, n_sp, heads, head_dim),
            out_shape=jax.ShapeDtypeStruct(latents.shape, bf16),
            in_specs=[any_spec, pl.BlockSpec(memory_space=pltpu.SMEM), pl.BlockSpec(memory_space=pltpu.VMEM)] + [any_spec] * 4,
            out_specs=any_spec,
            scratch_shapes=[
                pltpu.VMEM((width, 3 * width), bf16), pltpu.VMEM((width, width), bf16),
                pltpu.VMEM((width, hidden), bf16), pltpu.VMEM((hidden, width), bf16),
                pltpu.VMEM((2, rows, width), bf16), pltpu.VMEM((rows, 3 * width), bf16),
                pltpu.VMEM((rows, width), bf16), pltpu.VMEM((half, width), bf16), pltpu.VMEM((rows, width), bf16),
                pltpu.VMEM((half, hidden), bf16), pltpu.VMEM((steps, rows, width), bf16),
                pltpu.VMEM((videos, n_sp * frames, rows // n_sp, width), bf16), pltpu.VMEM((rows, rows), f32),
                dma((4,)), dma((2,)), dma((steps,)), dma((videos,)), dma, dma,
            ],
            compiler_params=pltpu.CompilerParams(collective_id=0, has_side_effects=True, vmem_limit_bytes=66_000_000),
            cost_estimate=pl.CostEstimate(
                flops=2 * 2 * tokens * width * (4 * width + 2 * hidden), bytes_accessed=70_000_000, transcendentals=0),
            name="dit",
        )(latents, valid_len, norm_w, w_qkv, w_out.reshape(2, width, width), w_up, w_down)

    return jax.shard_map(local_step, mesh=mesh, in_specs=(act_spec, P('data'), P(), P(), P(), P(), P()), out_specs=act_spec, check_vma=False)
```

```python
import functools
import math

import jax
import jax.numpy as jnp
from jax import lax
from jax.experimental import pallas as pl
from jax.experimental.pallas import tpu as pltpu
from jax.sharding import PartitionSpec as P

LN_EPS = 1e-6
MASKED = -1e30
OPEN = 3e38
LANES = 128
TILE = 256
SUB = 8
f32, bf16 = jnp.float32, jnp.bfloat16
MESH = pl.DeviceIdType.MESH


def layer_norm(tokens, gain, shift):
    values = tokens.astype(f32)
    inv_width = 1.0 / values.shape[-1]
    centered = values - jnp.sum(values, -1, keepdims=True) * inv_width
    variance = jnp.sum(centered * centered, -1, keepdims=True) * inv_width
    return (centered * lax.rsqrt(variance + LN_EPS) * gain + shift).astype(bf16)


def project(a, b):
    return jnp.dot(a, b, preferred_element_type=f32).astype(bf16)


def residual(base, delta):
    return (base.astype(f32) + delta.astype(f32)).astype(bf16)


def gelu(u):
    x = u.astype(f32)
    c = math.sqrt(2.0 / math.pi)
    half = 0.5 * x
    return (half + half * jnp.tanh(x * (x * x * (c * 0.044715) + c))).astype(bf16)


def head_windows(heads, head_dim):
    out = []
    for h in range(heads):
        lo = h * head_dim
        base = lo // LANES * LANES
        out.append((lo, base, LANES if lo + head_dim <= base + LANES else 2 * LANES))
    return out


def project_and_attend(norm_rows, nb, w, qkv, a_ref, heads, head_dim, groups, look, cap_ref):
    rows, width = nb.shape
    scale = head_dim ** -0.5 * math.log2(math.e)
    wins = head_windows(heads, head_dim)
    size = rows // groups
    piece = rows // 2
    queue = [(h, r) for h in range(heads) for r in range(0, rows, piece)]
    made = set()

    def lanes(h):
        _, base, w_ = wins[h]
        return lax.broadcasted_iota(jnp.int32, (1, w_), 1) + base

    def tiles(h, parts):
        _, base, w_ = wins[h]
        spans = [(p * width + base, p * width + base + w_ - 1) for p in parts]
        return list(dict.fromkeys(t for lo, hi in spans for t in range(lo // TILE, hi // TILE + 1)))

    def make(t, r):
        if (t, r) not in made:
            made.add((t, r))
            cols = slice(t * TILE, min((t + 1) * TILE, 3 * width))
            qkv[r:r + piece, cols] = project(nb[r:r + piece, :], w[:, cols])

    def need(h, parts):
        for t in tiles(h, parts):
            for r in range(0, rows, piece):
                make(t, r)

    order = list(dict.fromkeys(t for h in range(heads) for t in tiles(h, (0, 1, 2))))
    pieces = [(t, r) for t in order for r in range(0, rows, piece)]

    def scores(i):
        h, r = queue[i]
        need(h, (0, 1))
        lo, base, w_ = wins[h]
        lane = lanes(h)
        own = jnp.where((lane >= lo) & (lane < lo + head_dim), 1.0, 0.0).astype(bf16)
        q = qkv[r:r + piece, base:base + w_] * own
        k0 = r // size * size
        k = qkv[k0:k0 + size, width + base:width + base + w_]
        return lax.dot_general(q, k, (((1,), (1,)), ((), ())), preferred_element_type=f32)

    for r in range(0, rows, piece):
        norm_rows(r // piece)
        for t in tiles(0, (0, 1, 2)):
            make(t, r)
    ready = {i: scores(i) for i in range(look)}
    for i, (h, r) in enumerate(queue):
        if i + look < len(queue):
            ready[i + look] = scores(i + look)
        left = [u for u in pieces if u not in made]
        for u in left[:pl.cdiv(len(left), max(1, len(queue) - i - 2 * look))]:
            make(*u)
        need(h, (2,))
        lo, base, w_ = wins[h]
        k0 = r // size * size
        s = ready.pop(i) * scale
        if cap_ref is not None:
            s = jnp.minimum(s, cap_ref[...])
        e = jnp.exp2(s - jnp.max(s, -1, keepdims=True))
        p = (e * (1.0 / jnp.sum(e, -1, keepdims=True))).astype(bf16)
        o = project(p, qkv[k0:k0 + size, 2 * width + base:2 * width + base + w_])
        if lo != base:
            o = jnp.where(jnp.broadcast_to(lanes(h) >= lo, o.shape), o, a_ref[r:r + piece, base:base + w_])
        a_ref[r:r + piece, base:base + w_] = o


def kernel(n_sp, heads, head_dim, x_hbm, len_ref, norm_ref, wqkv_hbm, wout_hbm, wup_hbm, wdown_hbm, y_hbm,
           wqkv, wout, wup, wdown, xb, qkv, ab, hb, nb, ub, zb, rb, cap,
           w_sem, x_sem, send_sem, recv_sem, y_sem, own_sem):
    videos, frames, pairs, _, per_dev, width = x_hbm.shape
    rows = pairs * 2 * per_dev
    steps = videos * frames
    half = rows // 2
    groups = per_dev // SUB
    chunks = groups // 2
    me = lax.axis_index("sp")
    peers = n_sp - 1

    barrier = pltpu.get_barrier_semaphore()

    @pl.loop(1, n_sp)
    def _(k):
        pl.semaphore_signal(barrier, inc=1, device_id={"sp": lax.rem(me + k, n_sp)}, device_id_type=MESH)

    weights = ((wqkv_hbm, wqkv), (wout_hbm, wout), (wup_hbm, wup), (wdown_hbm, wdown))

    def load(i, layer):
        return pltpu.make_async_copy(weights[i][0].at[layer], weights[i][1], w_sem.at[i])

    def load_x(s, m):
        return pltpu.make_async_copy(
            x_hbm.at[s // frames, s % frames, :, m],
            xb.at[s % 2, m], x_sem.at[s % 2, m])

    for m in range(2):
        load_x(0, m).start()
    for i in range(4):
        load(i, 0).start()

    def frame_rows(s):
        return pl.ds(pl.multiple_of((me * frames + s % frames) * SUB, SUB), SUB)

    def send(s, m, pair):
        return pltpu.make_async_remote_copy(
            src_ref=zb.at[s, pl.ds((m * pairs + pair) * groups, groups)],
            dst_ref=rb.at[s // frames, :, frame_rows(s), :],
            send_sem=send_sem.at[s], recv_sem=recv_sem.at[s // frames],
            device_id={"sp": 2 * pair + m}, device_id_type=MESH)

    def result_rows(c, m):
        return pl.ds(pl.multiple_of(me * per_dev + (c % chunks * 2 + m) * SUB, SUB), SUB)

    def give(c, m, j):
        return pltpu.make_async_remote_copy(
            src_ref=zb.at[c, pl.ds((m * n_sp + j) * frames, frames)],
            dst_ref=y_hbm.at[c // chunks, :, result_rows(c, m), :],
            send_sem=send_sem.at[c], recv_sem=y_sem, device_id={"sp": j}, device_id_type=MESH)

    def keep(c, m):
        return pltpu.make_async_copy(
            zb.at[c, pl.ds((m * n_sp + me) * frames, frames)],
            y_hbm.at[c // chunks, :, result_rows(c, m), :], own_sem)

    def wait_sent(slot):
        sent = zb.at[slot, pl.ds(0, peers * groups)]
        pltpu.make_async_copy(sent, sent, send_sem.at[slot]).wait()

    @pl.loop(0, 2 * steps)
    def _(s):
        spatial = s < steps
        layer = s // steps
        slot = s % steps
        xs = xb.at[s % 2]

        @pl.when(spatial)
        def _():
            for m in range(2):
                load_x(s, m).wait()

        @pl.when(s + 1 < steps)
        def _():
            for m in range(2):
                load_x(s + 1, m).start()

        @pl.when(jnp.logical_and(s >= steps, slot % chunks == 0))
        def _():
            v = slot // chunks
            got = rb.at[v, :, pl.ds(0, peers * frames * SUB), :]
            pltpu.make_async_copy(got, got, recv_sem.at[v]).wait()
            shift = SUB.bit_length() - 1
            limit = len_ref[v]
            for r in range(0, half, LANES):
                qi = lax.broadcasted_iota(jnp.int32, (LANES, half), 0) + r
                ki = lax.broadcasted_iota(jnp.int32, (LANES, half), 1)
                kt = lax.shift_right_logical(ki, shift)
                ok = ((qi & (SUB - 1)) == (ki & (SUB - 1))) & (kt <= lax.shift_right_logical(qi, shift)) & (kt < limit)
                cap[r:r + LANES, :] = jnp.where(ok, OPEN, MASKED)

        @pl.when(slot == 0)
        def _():
            load(0, layer).wait()

        def norm_rows(m):
            norms = norm_ref[layer].astype(f32)
            nb[m * half:(m + 1) * half, :] = layer_norm(xs[m].reshape(half, width), norms[0:1], norms[1:2])

        @pl.when(spatial)
        def _():
            project_and_attend(norm_rows, nb, wqkv, qkv, ab, heads, head_dim, 1, 3, None)

        @pl.when(s >= steps)
        def _():
            for m in range(2):
                xs[m] = rb[slot // chunks, slot % chunks * 2 + m].reshape(pairs, per_dev, width)
            project_and_attend(norm_rows, nb, wqkv, qkv, ab, heads, head_dim, 2, 2, cap)

        @pl.when(s == steps - 1)
        def _():
            load(0, 1).start()

        @pl.when(slot == 0)
        def _():
            for i in range(1, 4):
                load(i, layer).wait()

        @pl.when(s >= steps)
        def _():
            wait_sent(slot)

        @pl.loop(0, 2)
        def _(m):
            at = pl.ds(pl.multiple_of(m * half, half), half)
            norms = norm_ref[layer].astype(f32)
            hb[...] = residual(xs[m].reshape(half, width), project(ab[at, :], wout[...]))
            nb[at, :] = layer_norm(hb[...], norms[2:3], norms[3:4])
            ub[...] = gelu(project(nb[at, :], wup[...]))
            z = residual(hb[...], project(ub[...], wdown[...]))
            zb[slot, pl.ds(m * (half // SUB), half // SUB)] = z.reshape(half // SUB, SUB, width)

            @pl.when(jnp.logical_and(s == 0, m == 0))
            def _():
                pl.semaphore_wait(barrier, peers)

            @pl.when(spatial)
            def _():
                @pl.loop(0, pairs)
                def _(k):
                    pair = lax.rem(me // 2 + k, pairs)

                    @pl.when(2 * pair + m != me)
                    def _():
                        send(s, m, pair).start()

                @pl.when(m == me % 2)
                def _():
                    for g in range(groups):
                        rb[s // frames, g, frame_rows(s), :] = zb[s, (m * pairs + me // 2) * groups + g]

            @pl.when(s >= steps)
            def _():
                @pl.loop(1, n_sp)
                def _(k):
                    give(slot, m, lax.rem(me + k, n_sp)).start()
                keep(slot, m).start()

        @pl.when(s == steps - 1)
        def _():
            for i in range(1, 4):
                load(i, 1).start()

    for slot in range(steps):
        wait_sent(slot)
    kept = y_hbm.at[:, :, pl.ds(0, per_dev), :]
    pltpu.make_async_copy(kept, kept, own_sem).wait()
    got = y_hbm.at[:, :, pl.ds(0, peers * per_dev), :]
    pltpu.make_async_copy(got, got, y_sem).wait()


def solution(mesh):
    act_spec = P('data', 'sp', None, None)
    n_sp = mesh.shape['sp']

    def local_step(latents, valid_len, norm_w, w_qkv, w_out, w_up, w_down):
        videos, frames, rows, width = latents.shape
        heads, head_dim = w_out.shape[1:3]
        hidden = w_up.shape[2]
        tokens = videos * frames * rows
        half = rows // 2
        any_spec = pl.BlockSpec(memory_space=pl.ANY)
        dma = pltpu.SemaphoreType.DMA
        steps = videos * frames
        return pl.pallas_call(
            functools.partial(kernel, n_sp, heads, head_dim),
            out_shape=jax.ShapeDtypeStruct(latents.shape, bf16),
            in_specs=[any_spec, pl.BlockSpec(memory_space=pltpu.SMEM), pl.BlockSpec(memory_space=pltpu.VMEM)] + [any_spec] * 4,
            out_specs=any_spec,
            scratch_shapes=[
                pltpu.VMEM((width, 3 * width), bf16), pltpu.VMEM((width, width), bf16),
                pltpu.VMEM((width, hidden), bf16), pltpu.VMEM((hidden, width), bf16),
                pltpu.VMEM((2, 2, n_sp // 2, rows // n_sp, width), bf16), pltpu.VMEM((rows, 3 * width), bf16),
                pltpu.VMEM((rows, width), bf16), pltpu.VMEM((half, width), bf16), pltpu.VMEM((rows, width), bf16),
                pltpu.VMEM((half, hidden), bf16), pltpu.VMEM((steps, rows // SUB, SUB, width), bf16),
                pltpu.VMEM((videos, rows // n_sp // SUB, n_sp * frames * SUB, width), bf16), pltpu.VMEM((half, half), f32),
                dma((4,)), dma((2, 2)), dma((steps,)), dma((videos,)), dma, dma,
            ],
            compiler_params=pltpu.CompilerParams(collective_id=0, has_side_effects=True, vmem_limit_bytes=66_000_000),
            cost_estimate=pl.CostEstimate(
                flops=2 * 2 * tokens * width * (4 * width + 2 * hidden), bytes_accessed=70_000_000, transcendentals=0),
            name="dit",
        )(latents.reshape(videos, frames, n_sp // 2, 2, rows // n_sp, width), valid_len, norm_w, w_qkv, w_out.reshape(2, width, width), w_up, w_down)

    return jax.shard_map(local_step, mesh=mesh, in_specs=(act_spec, P('data'), P(), P(), P(), P(), P()), out_specs=act_spec, check_vma=False)
```

```python
import functools
import math

import jax
import jax.numpy as jnp
from jax import lax
from jax.experimental import pallas as pl
from jax.experimental.pallas import tpu as pltpu
from jax.sharding import PartitionSpec as P

LN_EPS = 1e-6
MASKED = -1e30
OPEN = 3e38
LANES = 128
TILE = 256
SUB = 8
f32, bf16 = jnp.float32, jnp.bfloat16
MESH = pl.DeviceIdType.MESH


def layer_norm(tokens, gain, shift):
    values = tokens.astype(f32)
    inv_width = 1.0 / values.shape[-1]
    centered = values - jnp.sum(values, -1, keepdims=True) * inv_width
    variance = jnp.sum(centered * centered, -1, keepdims=True) * inv_width
    return (centered * lax.rsqrt(variance + LN_EPS) * gain + shift).astype(bf16)


def project(a, b):
    return jnp.dot(a, b, preferred_element_type=f32).astype(bf16)


def residual(base, delta):
    return (base.astype(f32) + delta.astype(f32)).astype(bf16)


def gelu(u):
    x = u.astype(f32)
    c = math.sqrt(2.0 / math.pi)
    half = 0.5 * x
    return (half + half * jnp.tanh(x * (x * x * (c * 0.044715) + c))).astype(bf16)


def head_windows(heads, head_dim):
    out = []
    for h in range(heads):
        lo = h * head_dim
        base = lo // LANES * LANES
        out.append((lo, base, LANES if lo + head_dim <= base + LANES else 2 * LANES))
    return out


def project_and_attend(norm_rows, nb, w, qkv, a_ref, heads, head_dim, groups, look, cap_ref):
    rows, width = nb.shape
    scale = head_dim ** -0.5 * math.log2(math.e)
    wins = head_windows(heads, head_dim)
    size = rows // groups
    piece = rows // 2
    queue = [(h, r) for h in range(heads) for r in range(0, rows, piece)]
    made = set()

    def lanes(h):
        _, base, w_ = wins[h]
        return lax.broadcasted_iota(jnp.int32, (1, w_), 1) + base

    def tiles(h, parts):
        _, base, w_ = wins[h]
        spans = [(p * width + base, p * width + base + w_ - 1) for p in parts]
        return list(dict.fromkeys(t for lo, hi in spans for t in range(lo // TILE, hi // TILE + 1)))

    def make(t, r):
        if (t, r) not in made:
            made.add((t, r))
            cols = slice(t * TILE, min((t + 1) * TILE, 3 * width))
            qkv[r:r + piece, cols] = project(nb[r:r + piece, :], w[:, cols])

    def need(h, parts):
        for t in tiles(h, parts):
            for r in range(0, rows, piece):
                make(t, r)

    order = list(dict.fromkeys(t for h in range(heads) for t in tiles(h, (0, 1, 2))))
    pieces = [(t, r) for t in order for r in range(0, rows, piece)]

    def scores(i):
        h, r = queue[i]
        need(h, (0, 1))
        lo, base, w_ = wins[h]
        lane = lanes(h)
        own = jnp.where((lane >= lo) & (lane < lo + head_dim), 1.0, 0.0).astype(bf16)
        q = qkv[r:r + piece, base:base + w_] * own
        k0 = r // size * size
        k = qkv[k0:k0 + size, width + base:width + base + w_]
        return lax.dot_general(q, k, (((1,), (1,)), ((), ())), preferred_element_type=f32)

    for r in range(0, rows, piece):
        norm_rows(r // piece)
        for t in tiles(0, (0, 1, 2)):
            make(t, r)
    ready = {i: scores(i) for i in range(look)}
    for i, (h, r) in enumerate(queue):
        if i + look < len(queue):
            ready[i + look] = scores(i + look)
        left = [u for u in pieces if u not in made]
        for u in left[:pl.cdiv(len(left), max(1, len(queue) - i - 2 * look))]:
            make(*u)
        need(h, (2,))
        lo, base, w_ = wins[h]
        k0 = r // size * size
        s = ready.pop(i) * scale
        if cap_ref is not None:
            s = jnp.minimum(s, cap_ref[...])
        e = jnp.exp2(s - jnp.max(s, -1, keepdims=True))
        p = (e * (1.0 / jnp.sum(e, -1, keepdims=True))).astype(bf16)
        o = project(p, qkv[k0:k0 + size, 2 * width + base:2 * width + base + w_])
        if lo != base:
            o = jnp.where(jnp.broadcast_to(lanes(h) >= lo, o.shape), o, a_ref[r:r + piece, base:base + w_])
        a_ref[r:r + piece, base:base + w_] = o


def kernel(n_sp, heads, head_dim, x_hbm, len_ref, norm_ref, wqkv_hbm, wout_hbm, wup_hbm, wdown_hbm, y_ref,
           wqkv, wout, wup, wdown, xb, qkv, ab, hb, nb, ub, zb, rb, cap,
           w_sem, x_sem, send_sem, recv_sem, y_sem):
    videos, frames, pairs, _, per_dev, width = x_hbm.shape
    rows = pairs * 2 * per_dev
    steps = videos * frames
    half = rows // 2
    groups = per_dev // SUB
    chunks = groups // 2
    me = lax.axis_index("sp")
    peers = n_sp - 1

    barrier = pltpu.get_barrier_semaphore()

    @pl.loop(1, n_sp)
    def _(k):
        pl.semaphore_signal(barrier, inc=1, device_id={"sp": lax.rem(me + k, n_sp)}, device_id_type=MESH)

    weights = ((wqkv_hbm, wqkv), (wout_hbm, wout), (wup_hbm, wup), (wdown_hbm, wdown))

    def load(i, layer):
        return pltpu.make_async_copy(weights[i][0].at[layer], weights[i][1], w_sem.at[i])

    def load_x(s, m):
        return pltpu.make_async_copy(
            x_hbm.at[s // frames, s % frames, :, m],
            xb.at[s % 2, m], x_sem.at[s % 2, m])

    for m in range(2):
        load_x(0, m).start()
    for i in range(4):
        load(i, 0).start()

    def frame_rows(s):
        return pl.ds(pl.multiple_of((me * frames + s % frames) * SUB, SUB), SUB)

    def send(s, m, pair):
        return pltpu.make_async_remote_copy(
            src_ref=zb.at[s, pl.ds((m * pairs + pair) * groups, groups)],
            dst_ref=rb.at[s // frames, :, frame_rows(s), :],
            send_sem=send_sem.at[s], recv_sem=recv_sem.at[s // frames],
            device_id={"sp": 2 * pair + m}, device_id_type=MESH)

    def result_rows(c, m):
        return pl.ds(pl.multiple_of(me * per_dev + (c % chunks * 2 + m) * SUB, SUB), SUB)

    def give(c, m, j):
        return pltpu.make_async_remote_copy(
            src_ref=zb.at[c, pl.ds((m * n_sp + j) * frames, frames)],
            dst_ref=y_ref.at[c // chunks, :, result_rows(c, m), :],
            send_sem=send_sem.at[c], recv_sem=y_sem, device_id={"sp": j}, device_id_type=MESH)

    def wait_sent(slot):
        sent = zb.at[slot, pl.ds(0, peers * groups)]
        pltpu.make_async_copy(sent, sent, send_sem.at[slot]).wait()

    @pl.loop(0, 2 * steps)
    def _(s):
        spatial = s < steps
        layer = s // steps
        slot = s % steps
        xs = xb.at[s % 2]

        @pl.when(spatial)
        def _():
            for m in range(2):
                load_x(s, m).wait()

        @pl.when(s + 1 < steps)
        def _():
            for m in range(2):
                load_x(s + 1, m).start()

        @pl.when(jnp.logical_and(s >= steps, slot % chunks == 0))
        def _():
            v = slot // chunks
            got = rb.at[v, :, pl.ds(0, peers * frames * SUB), :]
            pltpu.make_async_copy(got, got, recv_sem.at[v]).wait()
            shift = SUB.bit_length() - 1
            limit = len_ref[v]
            for r in range(0, half, LANES):
                qi = lax.broadcasted_iota(jnp.int32, (LANES, half), 0) + r
                ki = lax.broadcasted_iota(jnp.int32, (LANES, half), 1)
                kt = lax.shift_right_logical(ki, shift)
                ok = ((qi & (SUB - 1)) == (ki & (SUB - 1))) & (kt <= lax.shift_right_logical(qi, shift)) & (kt < limit)
                cap[r:r + LANES, :] = jnp.where(ok, OPEN, MASKED)

        @pl.when(slot == 0)
        def _():
            load(0, layer).wait()

        def norm_rows(m):
            norms = norm_ref[layer].astype(f32)
            nb[m * half:(m + 1) * half, :] = layer_norm(xs[m].reshape(half, width), norms[0:1], norms[1:2])

        @pl.when(spatial)
        def _():
            project_and_attend(norm_rows, nb, wqkv, qkv, ab, heads, head_dim, 1, 3, None)

        @pl.when(s >= steps)
        def _():
            for m in range(2):
                xs[m] = rb[slot // chunks, slot % chunks * 2 + m].reshape(pairs, per_dev, width)
            project_and_attend(norm_rows, nb, wqkv, qkv, ab, heads, head_dim, 2, 2, cap)

        @pl.when(s == steps - 1)
        def _():
            load(0, 1).start()

        @pl.when(slot == 0)
        def _():
            for i in range(1, 4):
                load(i, layer).wait()

        @pl.when(s >= steps)
        def _():
            wait_sent(slot)

        @pl.loop(0, 2)
        def _(m):
            at = pl.ds(pl.multiple_of(m * half, half), half)
            norms = norm_ref[layer].astype(f32)
            hb[...] = residual(xs[m].reshape(half, width), project(ab[at, :], wout[...]))
            nb[at, :] = layer_norm(hb[...], norms[2:3], norms[3:4])
            ub[...] = gelu(project(nb[at, :], wup[...]))
            z = residual(hb[...], project(ub[...], wdown[...]))
            zb[slot, pl.ds(m * (half // SUB), half // SUB)] = z.reshape(half // SUB, SUB, width)

            @pl.when(jnp.logical_and(s == 0, m == 0))
            def _():
                pl.semaphore_wait(barrier, peers)

            @pl.when(spatial)
            def _():
                @pl.loop(0, pairs)
                def _(k):
                    pair = lax.rem(me // 2 + k, pairs)

                    @pl.when(2 * pair + m != me)
                    def _():
                        send(s, m, pair).start()

                @pl.when(m == me % 2)
                def _():
                    for g in range(groups):
                        rb[s // frames, g, frame_rows(s), :] = zb[s, (m * pairs + me // 2) * groups + g]

            @pl.when(s >= steps)
            def _():
                @pl.loop(1, n_sp)
                def _(k):
                    give(slot, m, lax.rem(me + k, n_sp)).start()
                for f in range(frames):
                    y_ref[slot // chunks, f, result_rows(slot, m), :] = zb[slot, (m * n_sp + me) * frames + f]

        @pl.when(s == steps - 1)
        def _():
            for i in range(1, 4):
                load(i, 1).start()

    for slot in range(steps):
        wait_sent(slot)
    got = y_ref.at[:, :, pl.ds(0, peers * per_dev), :]
    pltpu.make_async_copy(got, got, y_sem).wait()


def solution(mesh):
    act_spec = P('data', 'sp', None, None)
    n_sp = mesh.shape['sp']

    def local_step(latents, valid_len, norm_w, w_qkv, w_out, w_up, w_down):
        videos, frames, rows, width = latents.shape
        heads, head_dim = w_out.shape[1:3]
        hidden = w_up.shape[2]
        tokens = videos * frames * rows
        half = rows // 2
        any_spec = pl.BlockSpec(memory_space=pl.ANY)
        dma = pltpu.SemaphoreType.DMA
        steps = videos * frames
        return pl.pallas_call(
            functools.partial(kernel, n_sp, heads, head_dim),
            out_shape=pltpu.VMEM(latents.shape, bf16),
            in_specs=[any_spec, pl.BlockSpec(memory_space=pltpu.SMEM), pl.BlockSpec(memory_space=pltpu.VMEM)] + [any_spec] * 4,
            out_specs=pl.BlockSpec(memory_space=pltpu.VMEM),
            scratch_shapes=[
                pltpu.VMEM((width, 3 * width), bf16), pltpu.VMEM((width, width), bf16),
                pltpu.VMEM((width, hidden), bf16), pltpu.VMEM((hidden, width), bf16),
                pltpu.VMEM((2, 2, n_sp // 2, rows // n_sp, width), bf16), pltpu.VMEM((rows, 3 * width), bf16),
                pltpu.VMEM((rows, width), bf16), pltpu.VMEM((half, width), bf16), pltpu.VMEM((rows, width), bf16),
                pltpu.VMEM((half, hidden), bf16), pltpu.VMEM((steps, rows // SUB, SUB, width), bf16),
                pltpu.VMEM((videos, rows // n_sp // SUB, n_sp * frames * SUB, width), bf16), pltpu.VMEM((half, half), f32),
                dma((4,)), dma((2, 2)), dma((steps,)), dma((videos,)), dma,
            ],
            compiler_params=pltpu.CompilerParams(collective_id=0, has_side_effects=True, vmem_limit_bytes=62_000_000),
            cost_estimate=pl.CostEstimate(
                flops=2 * 2 * tokens * width * (4 * width + 2 * hidden), bytes_accessed=70_000_000, transcendentals=0),
            name="dit",
        )(latents.reshape(videos, frames, n_sp // 2, 2, rows // n_sp, width), valid_len, norm_w, w_qkv, w_out.reshape(2, width, width), w_up, w_down)

    return jax.shard_map(local_step, mesh=mesh, in_specs=(act_spec, P('data'), P(), P(), P(), P(), P()), out_specs=act_spec, check_vma=False)
```

```python
import functools
import math

import jax
import jax.numpy as jnp
from jax import lax
from jax.experimental import pallas as pl
from jax.experimental.pallas import tpu as pltpu
from jax.sharding import PartitionSpec as P

LN_EPS = 1e-6
MASKED = -1e30
OPEN = 3e38
LANES = 128
TILE = 256
SUB = 8
f32, bf16 = jnp.float32, jnp.bfloat16
MESH = pl.DeviceIdType.MESH


def layer_norm(tokens, gain, shift):
    values = tokens.astype(f32)
    inv_width = 1.0 / values.shape[-1]
    centered = values - jnp.sum(values, -1, keepdims=True) * inv_width
    variance = jnp.sum(centered * centered, -1, keepdims=True) * inv_width
    return (centered * lax.rsqrt(variance + LN_EPS) * gain + shift).astype(bf16)


def project(a, b):
    return jnp.dot(a, b, preferred_element_type=f32).astype(bf16)


def residual(base, delta):
    return (base.astype(f32) + delta.astype(f32)).astype(bf16)


def gelu(u):
    x = u.astype(f32)
    c = math.sqrt(2.0 / math.pi)
    half = 0.5 * x
    return (half + half * jnp.tanh(x * (x * x * (c * 0.044715) + c))).astype(bf16)


def head_windows(heads, head_dim):
    out = []
    for h in range(heads):
        lo = h * head_dim
        base = lo // LANES * LANES
        out.append((lo, base, LANES if lo + head_dim <= base + LANES else 2 * LANES))
    return out


def column_tiles(wins, h, parts, width):
    _, base, w = wins[h]
    spans = [(p * width + base, p * width + base + w - 1) for p in parts]
    return list(dict.fromkeys(t for lo, hi in spans for t in range(lo // TILE, hi // TILE + 1)))


def columns(t, width):
    return slice(t * TILE, min((t + 1) * TILE, 3 * width))


def project_and_attend(nb, w, qkv, a_ref, heads, head_dim, groups, look, cap_ref):
    rows, width = 2 * nb.shape[1], nb.shape[2]
    scale = head_dim ** -0.5 * math.log2(math.e)
    wins = head_windows(heads, head_dim)
    size = rows // groups
    piece = rows // 2
    queue = [(h, r) for h in range(heads) for r in range(0, rows, piece)]
    def lanes(h):
        _, base, w_ = wins[h]
        return lax.broadcasted_iota(jnp.int32, (1, w_), 1) + base

    tiles = functools.partial(column_tiles, wins, width=width)
    made = {(t, r) for t in tiles(0, (0, 1, 2)) for r in range(0, rows, piece)}

    def make(t, r):
        if (t, r) not in made:
            made.add((t, r))
            cols = columns(t, width)
            qkv[r:r + piece, cols] = project(nb[r // piece], w[:, cols])

    def need(h, parts):
        for t in tiles(h, parts):
            for r in range(0, rows, piece):
                make(t, r)

    order = list(dict.fromkeys(t for h in range(heads) for t in tiles(h, (0, 1, 2))))
    pieces = [(t, r) for t in order for r in range(0, rows, piece)]

    def scores(i):
        h, r = queue[i]
        need(h, (0, 1))
        lo, base, w_ = wins[h]
        lane = lanes(h)
        own = jnp.where((lane >= lo) & (lane < lo + head_dim), 1.0, 0.0).astype(bf16)
        q = qkv[r:r + piece, base:base + w_] * own
        k0 = r // size * size
        k = qkv[k0:k0 + size, width + base:width + base + w_]
        return lax.dot_general(q, k, (((1,), (1,)), ((), ())), preferred_element_type=f32)

    ready = {i: scores(i) for i in range(look)}
    for i, (h, r) in enumerate(queue):
        if i + look < len(queue):
            ready[i + look] = scores(i + look)
        left = [u for u in pieces if u not in made]
        for u in left[:pl.cdiv(len(left), max(1, len(queue) - i - 2 * look))]:
            make(*u)
        need(h, (2,))
        lo, base, w_ = wins[h]
        k0 = r // size * size
        s = ready.pop(i) * scale
        if cap_ref is not None:
            s = jnp.minimum(s, cap_ref[...])
        e = jnp.exp2(s - jnp.max(s, -1, keepdims=True))
        p = (e * (1.0 / jnp.sum(e, -1, keepdims=True))).astype(bf16)
        o = project(p, qkv[k0:k0 + size, 2 * width + base:2 * width + base + w_])
        if lo != base:
            o = jnp.where(jnp.broadcast_to(lanes(h) >= lo, o.shape), o, a_ref[r:r + piece, base:base + w_])
        a_ref[r:r + piece, base:base + w_] = o


def kernel(n_sp, heads, head_dim, x_hbm, len_ref, norm_ref, wqkv_hbm, wout_hbm, wup_hbm, wdown_hbm, y_ref,
           wqkv, wfirst, wout, wup, wdown, xb, qkv, ab, hb, n1, n2, ub, zb, rb, cap,
           w_sem, first_sem, x_sem, send_sem, recv_sem, y_sem):
    videos, frames, pairs, _, per_dev, width = x_hbm.shape
    rows = pairs * 2 * per_dev
    steps = videos * frames
    half = rows // 2
    groups = per_dev // SUB
    chunks = groups // 2
    me = lax.axis_index("sp")
    peers = n_sp - 1

    barrier = pltpu.get_barrier_semaphore()

    @pl.loop(1, n_sp)
    def _(k):
        pl.semaphore_signal(barrier, inc=1, device_id={"sp": lax.rem(me + k, n_sp)}, device_id_type=MESH)

    weights = ((wqkv_hbm, wqkv), (wout_hbm, wout), (wup_hbm, wup), (wdown_hbm, wdown))

    def load(i, layer):
        return pltpu.make_async_copy(weights[i][0].at[layer], weights[i][1], w_sem.at[i])

    def load_x(s, m):
        return pltpu.make_async_copy(
            x_hbm.at[s // frames, s % frames, :, m],
            xb.at[s % 2, m], x_sem.at[s % 2, m])

    first = column_tiles(head_windows(heads, head_dim), 0, (0, 1, 2), width)

    def load_first(i, layer):
        return pltpu.make_async_copy(
            wqkv_hbm.at[layer, :, pl.ds(first[i] * TILE, TILE)], wfirst.at[i], first_sem.at[i])

    def norm_next(layer, s, m):
        norms = norm_ref[layer].astype(f32)
        n1[m] = layer_norm(xb[s % 2, m].reshape(half, width), norms[0:1], norms[1:2])

    def project_first(m):
        for i, t in enumerate(first):
            qkv[pl.ds(pl.multiple_of(m * half, half), half), columns(t, width)] = project(n1[m], wfirst[i])

    for m in range(2):
        load_x(0, m).start()
    for i in range(len(first)):
        load_first(i, 0).start()
    for i in range(4):
        load(i, 0).start()
    for m in range(2):
        load_x(1, m).start()

    def frame_rows(s):
        return pl.ds(pl.multiple_of((me * frames + s % frames) * SUB, SUB), SUB)

    def send(s, m, pair):
        return pltpu.make_async_remote_copy(
            src_ref=zb.at[s, pl.ds((m * pairs + pair) * groups, groups)],
            dst_ref=rb.at[s // frames, :, frame_rows(s), :],
            send_sem=send_sem.at[s], recv_sem=recv_sem.at[s // frames],
            device_id={"sp": 2 * pair + m}, device_id_type=MESH)

    def result_rows(c, m):
        return pl.ds(pl.multiple_of(me * per_dev + (c % chunks * 2 + m) * SUB, SUB), SUB)

    def give(c, m, j):
        return pltpu.make_async_remote_copy(
            src_ref=zb.at[c, pl.ds((m * n_sp + j) * frames, frames)],
            dst_ref=y_ref.at[c // chunks, :, result_rows(c, m), :],
            send_sem=send_sem.at[c], recv_sem=y_sem, device_id={"sp": j}, device_id_type=MESH)

    def wait_sent(slot):
        sent = zb.at[slot, pl.ds(0, peers * groups)]
        pltpu.make_async_copy(sent, sent, send_sem.at[slot]).wait()

    for m in range(2):
        load_x(0, m).wait()
    for i in range(len(first)):
        load_first(i, 0).wait()
    for m in range(2):
        norm_next(0, 0, m)
        project_first(m)
    load(0, 0).wait()

    @pl.loop(0, 2 * steps)
    def _(s):
        spatial = s < steps
        layer = s // steps
        slot = s % steps
        xs = xb.at[s % 2]

        @pl.when(spatial)
        def _():
            project_and_attend(n1, wqkv, qkv, ab, heads, head_dim, 1, 3, None)

        @pl.when(s >= steps)
        def _():
            project_and_attend(n1, wqkv, qkv, ab, heads, head_dim, 2, 2, cap)

        @pl.when(s == steps - 1)
        def _():
            load(0, 1).start()
            for i in range(len(first)):
                load_first(i, 1).wait()

        @pl.when(slot == 0)
        def _():
            for i in range(1, 4):
                load(i, layer).wait()

        @pl.when(s >= steps)
        def _():
            wait_sent(slot)

        @pl.when(s + 1 < steps)
        def _():
            for m in range(2):
                load_x(s + 1, m).wait()

        @pl.when(jnp.logical_and(s + 1 >= steps, s + 1 < 2 * steps))
        def _():
            c = s + 1 - steps

            @pl.when(c % chunks == 0)
            def _():
                v = c // chunks
                got = rb.at[v, :, pl.ds(0, peers * frames * SUB), :]
                pltpu.make_async_copy(got, got, recv_sem.at[v]).wait()
                shift = SUB.bit_length() - 1
                limit = len_ref[v]
                for r in range(0, half, LANES):
                    qi = lax.broadcasted_iota(jnp.int32, (LANES, half), 0) + r
                    ki = lax.broadcasted_iota(jnp.int32, (LANES, half), 1)
                    kt = lax.shift_right_logical(ki, shift)
                    ok = ((qi & (SUB - 1)) == (ki & (SUB - 1))) & (kt <= lax.shift_right_logical(qi, shift)) & (kt < limit)
                    cap[r:r + LANES, :] = jnp.where(ok, OPEN, MASKED)

            for m in range(2):
                xb[(s + 1) % 2, m] = rb[c // chunks, c % chunks * 2 + m].reshape(pairs, per_dev, width)

        @pl.loop(0, 2)
        def _(m):
            at = pl.ds(pl.multiple_of(m * half, half), half)
            norms = norm_ref[layer].astype(f32)
            norm_next((s + 1) % (2 * steps) // steps, s + 1, m)
            hb[...] = residual(xs[m].reshape(half, width), project(ab[at, :], wout[...]))
            project_first(m)
            n2[...] = layer_norm(hb[...], norms[2:3], norms[3:4])
            ub[...] = gelu(project(n2[...], wup[...]))
            z = residual(hb[...], project(ub[...], wdown[...]))
            zb[slot, pl.ds(m * (half // SUB), half // SUB)] = z.reshape(half // SUB, SUB, width)

            @pl.when(jnp.logical_and(s == 0, m == 0))
            def _():
                pl.semaphore_wait(barrier, peers)

            @pl.when(spatial)
            def _():
                @pl.loop(0, pairs)
                def _(k):
                    pair = lax.rem(me // 2 + k, pairs)

                    @pl.when(2 * pair + m != me)
                    def _():
                        send(s, m, pair).start()

                @pl.when(m == me % 2)
                def _():
                    for g in range(groups):
                        rb[s // frames, g, frame_rows(s), :] = zb[s, (m * pairs + me // 2) * groups + g]

            @pl.when(s >= steps)
            def _():
                @pl.loop(1, n_sp)
                def _(k):
                    give(slot, m, lax.rem(me + k, n_sp)).start()
                for f in range(frames):
                    y_ref[slot // chunks, f, result_rows(slot, m), :] = zb[slot, (m * n_sp + me) * frames + f]

        @pl.when(s == steps - 1)
        def _():
            load(0, 1).wait()
            for i in range(1, 4):
                load(i, 1).start()

        @pl.when(s == steps - 2)
        def _():
            for i in range(len(first)):
                load_first(i, 1).start()

        @pl.when(s + 2 < steps)
        def _():
            for m in range(2):
                load_x(s + 2, m).start()

    for slot in range(steps):
        wait_sent(slot)
    got = y_ref.at[:, :, pl.ds(0, peers * per_dev), :]
    pltpu.make_async_copy(got, got, y_sem).wait()


def solution(mesh):
    act_spec = P('data', 'sp', None, None)
    n_sp = mesh.shape['sp']

    def local_step(latents, valid_len, norm_w, w_qkv, w_out, w_up, w_down):
        videos, frames, rows, width = latents.shape
        heads, head_dim = w_out.shape[1:3]
        hidden = w_up.shape[2]
        tokens = videos * frames * rows
        half = rows // 2
        any_spec = pl.BlockSpec(memory_space=pl.ANY)
        dma = pltpu.SemaphoreType.DMA
        steps = videos * frames
        firsts = len(column_tiles(head_windows(heads, head_dim), 0, (0, 1, 2), width))
        return pl.pallas_call(
            functools.partial(kernel, n_sp, heads, head_dim),
            out_shape=pltpu.VMEM(latents.shape, bf16),
            in_specs=[any_spec, pl.BlockSpec(memory_space=pltpu.SMEM), pl.BlockSpec(memory_space=pltpu.VMEM)] + [any_spec] * 4,
            out_specs=pl.BlockSpec(memory_space=pltpu.VMEM),
            scratch_shapes=[
                pltpu.VMEM((width, 3 * width), bf16), pltpu.VMEM((firsts, width, TILE), bf16),
                pltpu.VMEM((width, width), bf16),
                pltpu.VMEM((width, hidden), bf16), pltpu.VMEM((hidden, width), bf16),
                pltpu.VMEM((2, 2, n_sp // 2, rows // n_sp, width), bf16), pltpu.VMEM((rows, 3 * width), bf16),
                pltpu.VMEM((rows, width), bf16), pltpu.VMEM((half, width), bf16),
                pltpu.VMEM((2, half, width), bf16), pltpu.VMEM((half, width), bf16),
                pltpu.VMEM((half, hidden), bf16), pltpu.VMEM((steps, rows // SUB, SUB, width), bf16),
                pltpu.VMEM((videos, rows // n_sp // SUB, n_sp * frames * SUB, width), bf16), pltpu.VMEM((half, half), f32),
                dma((4,)), dma((firsts,)), dma((2, 2)), dma((steps,)), dma((videos,)), dma,
            ],
            compiler_params=pltpu.CompilerParams(collective_id=0, has_side_effects=True, vmem_limit_bytes=62_000_000),
            cost_estimate=pl.CostEstimate(
                flops=2 * 2 * tokens * width * (4 * width + 2 * hidden), bytes_accessed=70_000_000, transcendentals=0),
            name="dit",
        )(latents.reshape(videos, frames, n_sp // 2, 2, rows // n_sp, width), valid_len, norm_w, w_qkv, w_out.reshape(2, width, width), w_up, w_down)

    return jax.shard_map(local_step, mesh=mesh, in_specs=(act_spec, P('data'), P(), P(), P(), P(), P()), out_specs=act_spec, check_vma=False)
```

```python
import functools
import math

import jax
import jax.numpy as jnp
from jax import lax
from jax.experimental import pallas as pl
from jax.experimental.pallas import tpu as pltpu
from jax.sharding import PartitionSpec as P

LN_EPS = 1e-6
MASKED = -1e30
OPEN = 3e38
LANES = 128
TILE = 256
SUB = 8
PACK = 16
f32, bf16 = jnp.float32, jnp.bfloat16
MESH = pl.DeviceIdType.MESH


def layer_norm(tokens, gain, shift):
    values = tokens.astype(f32)
    inv_width = 1.0 / values.shape[-1]
    centered = values - jnp.sum(values, -1, keepdims=True) * inv_width
    variance = jnp.sum(centered * centered, -1, keepdims=True) * inv_width
    return (centered * lax.rsqrt(variance + LN_EPS) * gain + shift).astype(bf16)


def project(a, b):
    return jnp.dot(a, b, preferred_element_type=f32).astype(bf16)


def residual(base, delta):
    return (base.astype(f32) + delta.astype(f32)).astype(bf16)


def gelu(u):
    x = u.astype(f32)
    c = math.sqrt(2.0 / math.pi)
    half = 0.5 * x
    return (half + half * jnp.tanh(x * (x * x * (c * 0.044715) + c))).astype(bf16)


def head_windows(heads, head_dim):
    out = []
    for h in range(heads):
        lo = h * head_dim
        base = lo // LANES * LANES
        out.append((lo, base, LANES if lo + head_dim <= base + LANES else 2 * LANES))
    return out


def column_tiles(wins, h, parts, width):
    _, base, w = wins[h]
    spans = [(p * width + base, p * width + base + w - 1) for p in parts]
    return list(dict.fromkeys(t for lo, hi in spans for t in range(lo // TILE, hi // TILE + 1)))


def columns(t, width):
    return slice(t * TILE, min((t + 1) * TILE, 3 * width))


def attend(nb, w_of, qk, vt, a_ref, heads, head_dim, mine, key_halves, made, look, lead, cap_ref):
    _, half, width = nb.shape
    scale = head_dim ** -0.5 * math.log2(math.e)
    wins = head_windows(heads, head_dim)
    made = set(made)
    key_rows = slice(key_halves[0] * half, (key_halves[-1] + 1) * half)

    def pieces(h, parts):
        return [(t, r) for p in parts for t in column_tiles(wins, h, (p,), width) for r in ((mine,) if p == 0 else key_halves)]

    def make(t, r):
        if (t, r) not in made:
            made.add((t, r))
            project_piece(nb, w_of(t), qk, vt, t, r)

    def keys(cols):
        return jnp.concatenate([qk[r, :, cols] for r in key_halves], axis=0)

    def scores(h):
        for u in pieces(h, (0, 1)):
            make(*u)
        lo, base, w_ = wins[h]
        lane = lax.broadcasted_iota(jnp.int32, (1, w_), 1) + base
        own = jnp.where((lane >= lo) & (lane < lo + head_dim), 1.0, 0.0).astype(bf16)
        q = qk[mine, :, base:base + w_] * own
        k = keys(slice(width + base, width + base + w_))
        return lax.dot_general(k, q, (((1,), (1,)), ((), ())), preferred_element_type=f32)

    due = []
    for h in range(heads):
        for p, step in ((0, h - look), (1, h - look), (2, h)):
            due += [(max(step, -1), u) for u in pieces(h, (p,))]
    ready = {h: scores(h) for h in range(look)}
    done, parts = 0, []
    for h in range(heads):
        for step, u in sorted(due, key=lambda d: d[0]):
            if step <= h + lead:
                make(*u)
        if h + look < heads:
            ready[h + look] = scores(h + look)
        s = ready.pop(h)
        if cap_ref is not None:
            s = jnp.minimum(s, cap_ref[...])
        e = jnp.exp2((s - jnp.max(s, 0, keepdims=True)) * scale)
        p = (e * (1.0 / jnp.sum(e, 0, keepdims=True))).astype(bf16)
        lo = h * head_dim
        r0, r1 = lo // PACK * PACK, pl.cdiv(lo + head_dim, PACK) * PACK
        o = jnp.dot(vt[r0:r1, key_rows], p, preferred_element_type=f32)
        parts.append((lo, o[lo - r0:lo - r0 + head_dim, :]))
        while (done + 1) * LANES <= lo + head_dim:
            g0, g1 = done * LANES, (done + 1) * LANES
            rows = [x[max(g0 - l, 0):min(g1 - l, head_dim), :] for l, x in parts if l < g1]
            a_ref[:, g0:g1] = jnp.concatenate(rows, axis=0).astype(bf16).T
            parts = [(l, x) for l, x in parts if l + head_dim > g1]
            done += 1


def project_piece(nb, w, qk, vt, t, r):
    half, width = nb.shape[1:]
    piece = project(nb[r], w)
    cols = columns(t, width)
    if cols.start < 2 * width:
        qk[r, :, cols] = piece
    else:
        vt[cols.start - 2 * width:cols.stop - 2 * width, r * half:(r + 1) * half] = piece.T


def kernel(n_sp, heads, head_dim, x_hbm, len_ref, norm_ref, wqkv_hbm, wout_hbm, wup_hbm, wdown_hbm, y_ref,
           wrest, wfirst, wout, wup, wdown, xb, qk, vt, ab, hb, n1, ub, zb, rb, cap,
           w_sem, rest_sem, first_sem, x_sem, send_sem, recv_sem, y_sem):
    videos, frames, pairs, _, per_dev, width = x_hbm.shape
    rows = pairs * 2 * per_dev
    steps = videos * frames
    half = rows // 2
    groups = per_dev // SUB
    chunks = groups // 2
    me = lax.axis_index("sp")
    peers = n_sp - 1

    barrier = pltpu.get_barrier_semaphore()

    @pl.loop(1, n_sp)
    def _(k):
        pl.semaphore_signal(barrier, inc=1, device_id={"sp": lax.rem(me + k, n_sp)}, device_id_type=MESH)

    weights = ((wout_hbm, wout), (wup_hbm, wup), (wdown_hbm, wdown))

    def load(i, layer):
        return pltpu.make_async_copy(weights[i][0].at[layer], weights[i][1], w_sem.at[i])

    def load_x(s, m):
        return pltpu.make_async_copy(
            x_hbm.at[s // frames, s % frames, :, m], xb.at[s % 2, m], x_sem.at[s % 2, m])

    tiles = pl.cdiv(3 * width, TILE)
    first = column_tiles(head_windows(heads, head_dim), 0, (0, 1, 2), width)
    rest = [t for t in range(tiles) if t not in first]
    extra = [t for t in range(width // TILE) if t not in first]

    def load_tile(t, layer):
        cols = columns(t, width)
        home, sem = (wfirst.at[first.index(t)], first_sem) if t in first else (wrest.at[rest.index(t)], rest_sem)
        size = cols.stop - cols.start
        return pltpu.make_async_copy(
            wqkv_hbm.at[layer, :, pl.ds(cols.start, size)], home.at[:, pl.ds(0, size)],
            sem.at[(first if t in first else rest).index(t)])

    def w_of(t):
        cols = columns(t, width)
        size = cols.stop - cols.start
        return wfirst[first.index(t)] if t in first else wrest[rest.index(t), :, :size]

    def norm_next(layer, s, m):
        norms = norm_ref[layer].astype(f32)
        n1[m] = layer_norm(xb[s % 2, m].reshape(half, width), norms[0:1], norms[1:2])

    def project_first(m):
        for t in first:
            project_piece(n1, w_of(t), qk, vt, t, m)

    for m in range(2):
        load_x(0, m).start()
    for t in first + rest:
        load_tile(t, 0).start()
    for i in range(3):
        load(i, 0).start()
    for m in range(2):
        load_x(1, m).start()

    def frame_rows(s):
        return pl.ds(pl.multiple_of((me * frames + s % frames) * SUB, SUB), SUB)

    def send(s, m, pair):
        return pltpu.make_async_remote_copy(
            src_ref=zb.at[s, pl.ds((m * pairs + pair) * groups, groups)],
            dst_ref=rb.at[s // frames, :, frame_rows(s), :],
            send_sem=send_sem.at[s], recv_sem=recv_sem.at[s // frames],
            device_id={"sp": 2 * pair + m}, device_id_type=MESH)

    def result_rows(c, m):
        return pl.ds(pl.multiple_of(me * per_dev + (c % chunks * 2 + m) * SUB, SUB), SUB)

    def give(c, m, j):
        return pltpu.make_async_remote_copy(
            src_ref=zb.at[c, pl.ds((m * n_sp + j) * frames, frames)],
            dst_ref=y_ref.at[c // chunks, :, result_rows(c, m), :],
            send_sem=send_sem.at[c], recv_sem=y_sem, device_id={"sp": j}, device_id_type=MESH)

    def wait_sent(slot):
        sent = zb.at[slot, pl.ds(0, peers * groups)]
        pltpu.make_async_copy(sent, sent, send_sem.at[slot]).wait()

    for m in range(2):
        load_x(0, m).wait()
    for t in first:
        load_tile(t, 0).wait()
    for m in range(2):
        norm_next(0, 0, m)
        project_first(m)
    for t in rest:
        load_tile(t, 0).wait()

    @pl.loop(0, 2 * steps)
    def _(s):
        spatial = s < steps
        temporal = s >= steps
        layer = s // steps
        slot = s % steps
        xs = xb.at[s % 2]
        attention = functools.partial(attend, n1, w_of, qk, vt, ab, heads, head_dim)
        there = {(t, r) for t in first for r in range(2)}

        def out(m):
            hb[...] = residual(xs[m].reshape(half, width), project(ab[...], wout[...]))

        def norm():
            norms = norm_ref[layer].astype(f32)
            ab[...] = layer_norm(hb[...], norms[2:3], norms[3:4])

        def up():
            ub[...] = gelu(project(ab[...], wup[...]))

        def down(m):
            z = residual(hb[...], project(ub[...], wdown[...]))
            zb[slot, m * (half // SUB):(m + 1) * (half // SUB)] = z.reshape(half // SUB, SUB, width)

        def deliver(m):
            @pl.when(spatial)
            def _():
                @pl.loop(0, pairs)
                def _(k):
                    pair = lax.rem(me // 2 + k, pairs)

                    @pl.when(2 * pair + m != me)
                    def _():
                        send(s, m, pair).start()

                @pl.when(m == me % 2)
                def _():
                    for g in range(groups):
                        rb[s // frames, g, frame_rows(s), :] = zb[s, (m * pairs + me // 2) * groups + g]

            @pl.when(temporal)
            def _():
                @pl.loop(1, n_sp)
                def _(k):
                    give(slot, m, lax.rem(me + k, n_sp)).start()
                for f in range(frames):
                    y_ref[slot // chunks, f, result_rows(slot, m), :] = zb[slot, (m * n_sp + me) * frames + f]

        @pl.when(spatial)
        def _():
            attention(0, (0, 1), there, 3, 2, None)

        @pl.when(temporal)
        def _():
            attention(0, (0,), there, 3, 3, cap)

        @pl.when(slot == 0)
        def _():
            for i in range(3):
                load(i, layer).wait()

        @pl.when(temporal)
        def _():
            wait_sent(slot)

        out(0)
        for t in extra:
            project_piece(n1, w_of(t), qk, vt, t, 1)
        norm()
        up()
        down(0)

        @pl.when(s == 0)
        def _():
            pl.semaphore_wait(barrier, peers)

        deliver(0)

        @pl.when(spatial)
        def _():
            attention(1, (0, 1), {(t, r) for t in range(tiles) for r in range(2)}, 5, 3, None)

        @pl.when(temporal)
        def _():
            attention(1, (1,), there | {(t, 1) for t in extra}, 4, 3, cap)

        @pl.when(s == steps - 1)
        def _():
            for t in rest:
                load_tile(t, 1).start()
            for t in first:
                load_tile(t, 1).wait()

        @pl.when(s + 1 < steps)
        def _():
            for m in range(2):
                load_x(s + 1, m).wait()

        @pl.when(jnp.logical_and(s + 1 >= steps, s + 1 < 2 * steps))
        def _():
            c = s + 1 - steps

            @pl.when(c % chunks == 0)
            def _():
                v = c // chunks
                got = rb.at[v, :, pl.ds(0, peers * frames * SUB), :]
                pltpu.make_async_copy(got, got, recv_sem.at[v]).wait()
                shift = SUB.bit_length() - 1
                limit = len_ref[v]
                for r in range(0, half, LANES):
                    ki = lax.broadcasted_iota(jnp.int32, (LANES, half), 0) + r
                    qi = lax.broadcasted_iota(jnp.int32, (LANES, half), 1)
                    kt = lax.shift_right_logical(ki, shift)
                    ok = ((qi & (SUB - 1)) == (ki & (SUB - 1))) & (kt <= lax.shift_right_logical(qi, shift)) & (kt < limit)
                    cap[r:r + LANES, :] = jnp.where(ok, OPEN, MASKED)

            for m in range(2):
                xb[(s + 1) % 2, m] = rb[c // chunks, c % chunks * 2 + m].reshape(pairs, per_dev, width)

        after = (s + 1) % (2 * steps) // steps
        norm_next(after, s + 1, 0)
        out(1)
        project_first(0)
        norm()
        up()
        norm_next(after, s + 1, 1)
        project_first(1)
        down(1)
        deliver(1)

        @pl.when(s == steps - 1)
        def _():
            for t in rest:
                load_tile(t, 1).wait()
            for i in range(3):
                load(i, 1).start()

        @pl.when(s == steps - 2)
        def _():
            for t in first:
                load_tile(t, 1).start()

        @pl.when(s + 2 < steps)
        def _():
            for m in range(2):
                load_x(s + 2, m).start()

    for slot in range(steps):
        wait_sent(slot)
    got = y_ref.at[:, :, pl.ds(0, peers * per_dev), :]
    pltpu.make_async_copy(got, got, y_sem).wait()


def solution(mesh):
    act_spec = P('data', 'sp', None, None)
    n_sp = mesh.shape['sp']

    def local_step(latents, valid_len, norm_w, w_qkv, w_out, w_up, w_down):
        videos, frames, rows, width = latents.shape
        heads, head_dim = w_out.shape[1:3]
        hidden = w_up.shape[2]
        tokens = videos * frames * rows
        half = rows // 2
        any_spec = pl.BlockSpec(memory_space=pl.ANY)
        dma = pltpu.SemaphoreType.DMA
        steps = videos * frames
        firsts = len(column_tiles(head_windows(heads, head_dim), 0, (0, 1, 2), width))
        rests = pl.cdiv(3 * width, TILE) - firsts
        return pl.pallas_call(
            functools.partial(kernel, n_sp, heads, head_dim),
            out_shape=pltpu.VMEM(latents.shape, bf16),
            in_specs=[any_spec, pl.BlockSpec(memory_space=pltpu.SMEM), pl.BlockSpec(memory_space=pltpu.VMEM)] + [any_spec] * 4,
            out_specs=pl.BlockSpec(memory_space=pltpu.VMEM),
            scratch_shapes=[
                pltpu.VMEM((rests, width, TILE), bf16), pltpu.VMEM((firsts, width, TILE), bf16),
                pltpu.VMEM((width, width), bf16),
                pltpu.VMEM((width, hidden), bf16), pltpu.VMEM((hidden, width), bf16),
                pltpu.VMEM((2, 2, n_sp // 2, rows // n_sp, width), bf16), pltpu.VMEM((2, half, 2 * width), bf16),
                pltpu.VMEM((width, rows), bf16),
                pltpu.VMEM((half, width), bf16), pltpu.VMEM((half, width), bf16),
                pltpu.VMEM((2, half, width), bf16),
                pltpu.VMEM((half, hidden), bf16), pltpu.VMEM((steps, rows // SUB, SUB, width), bf16),
                pltpu.VMEM((videos, rows // n_sp // SUB, n_sp * frames * SUB, width), bf16), pltpu.VMEM((half, half), f32),
                dma((3,)), dma((rests,)), dma((firsts,)), dma((2, 2)), dma((steps,)), dma((videos,)), dma,
            ],
            compiler_params=pltpu.CompilerParams(collective_id=0, has_side_effects=True, vmem_limit_bytes=62_000_000),
            cost_estimate=pl.CostEstimate(
                flops=2 * 2 * tokens * width * (4 * width + 2 * hidden), bytes_accessed=70_000_000, transcendentals=0),
            name="dit",
        )(latents.reshape(videos, frames, n_sp // 2, 2, rows // n_sp, width), valid_len, norm_w, w_qkv, w_out.reshape(2, width, width), w_up, w_down)

    return jax.shard_map(local_step, mesh=mesh, in_specs=(act_spec, P('data'), P(), P(), P(), P(), P()), out_specs=act_spec, check_vma=False)
```

```python
import functools
import math

import jax
import jax.numpy as jnp
from jax import lax
from jax.experimental import pallas as pl
from jax.experimental.pallas import tpu as pltpu
from jax.sharding import PartitionSpec as P

LN_EPS = 1e-6
MASKED = -1e30
OPEN = 3e38
LANES = 128
TILE = 256
SUB = 8
PACK = 16
f32, bf16 = jnp.float32, jnp.bfloat16
MESH = pl.DeviceIdType.MESH


def layer_norm(tokens, gain, shift):
    values = tokens.astype(f32)
    inv_width = 1.0 / values.shape[-1]
    centered = values - jnp.sum(values, -1, keepdims=True) * inv_width
    variance = jnp.sum(centered * centered, -1, keepdims=True) * inv_width
    return (centered * lax.rsqrt(variance + LN_EPS) * gain + shift).astype(bf16)


def project(a, b):
    return jnp.dot(a, b, preferred_element_type=f32).astype(bf16)


def residual(base, delta):
    return (base.astype(f32) + delta.astype(f32)).astype(bf16)


def gelu(u):
    x = u.astype(f32)
    c = math.sqrt(2.0 / math.pi)
    half = 0.5 * x
    return (half + half * jnp.tanh(x * (x * x * (c * 0.044715) + c))).astype(bf16)


def head_windows(heads, head_dim):
    out = []
    for h in range(heads):
        lo = h * head_dim
        base = lo // LANES * LANES
        out.append((lo, base, LANES if lo + head_dim <= base + LANES else 2 * LANES))
    return out


def column_tiles(wins, h, parts, width):
    _, base, w = wins[h]
    spans = [(p * width + base, p * width + base + w - 1) for p in parts]
    return list(dict.fromkeys(t for lo, hi in spans for t in range(lo // TILE, hi // TILE + 1)))


def columns(t, width):
    return slice(t * TILE, min((t + 1) * TILE, 3 * width))


def attend(nb, w_of, qk, vt, a_ref, heads, head_dim, mine, key_halves, made, look, lead, cap_ref):
    _, half, width = nb.shape
    scale = head_dim ** -0.5 * math.log2(math.e)
    wins = head_windows(heads, head_dim)
    made = set(made)
    key_rows = slice(key_halves[0] * half, (key_halves[-1] + 1) * half)

    def pieces(h, parts):
        return [(t, r) for p in parts for t in column_tiles(wins, h, (p,), width) for r in ((mine,) if p == 0 else key_halves)]

    def make(t, r):
        if (t, r) not in made:
            made.add((t, r))
            project_piece(nb, w_of(t), qk, vt, t, r)

    def keys(cols):
        return jnp.concatenate([qk[r, :, cols] for r in key_halves], axis=0)

    def scores(h):
        for u in pieces(h, (0, 1)):
            make(*u)
        lo, base, w_ = wins[h]
        lane = lax.broadcasted_iota(jnp.int32, (1, w_), 1) + base
        own = jnp.where((lane >= lo) & (lane < lo + head_dim), 1.0, 0.0).astype(bf16)
        q = qk[mine, :, base:base + w_] * own
        k = keys(slice(width + base, width + base + w_))
        return lax.dot_general(k, q, (((1,), (1,)), ((), ())), preferred_element_type=f32)

    due = []
    for h in range(heads):
        for p, step in ((0, h - look), (1, h - look), (2, h)):
            due += [(max(step, -1), u) for u in pieces(h, (p,))]
    ready = {h: scores(h) for h in range(look)}
    done, parts = 0, []
    for h in range(heads):
        for step, u in sorted(due, key=lambda d: d[0]):
            if step <= h + lead:
                make(*u)
        if h + look < heads:
            ready[h + look] = scores(h + look)
        s = ready.pop(h)
        if cap_ref is not None:
            s = jnp.minimum(s, cap_ref[...])
        e = jnp.exp2((s - jnp.max(s, 0, keepdims=True)) * scale)
        p = (e * (1.0 / jnp.sum(e, 0, keepdims=True))).astype(bf16)
        lo = h * head_dim
        r0, r1 = lo // PACK * PACK, pl.cdiv(lo + head_dim, PACK) * PACK
        o = jnp.dot(vt[r0:r1, key_rows], p, preferred_element_type=f32)
        parts.append((lo, o[lo - r0:lo - r0 + head_dim, :]))
        while (done + 1) * LANES <= lo + head_dim:
            g0, g1 = done * LANES, (done + 1) * LANES
            rows = [x[max(g0 - l, 0):min(g1 - l, head_dim), :] for l, x in parts if l < g1]
            a_ref[:, g0:g1] = jnp.concatenate(rows, axis=0).astype(bf16).T
            parts = [(l, x) for l, x in parts if l + head_dim > g1]
            done += 1


def project_piece(nb, w, qk, vt, t, r):
    half, width = nb.shape[1:]
    piece = project(nb[r], w)
    cols = columns(t, width)
    if cols.start < 2 * width:
        qk[r, :, cols] = piece
    else:
        vt[cols.start - 2 * width:cols.stop - 2 * width, r * half:(r + 1) * half] = piece.T


def kernel(n_sp, heads, head_dim, x_hbm, len_ref, norm_ref, wqkv_hbm, wout_hbm, wup_hbm, wdown_hbm, y_ref,
           wrest, wfirst, wout, wup, wdown, xb, qk, vt, ab, hb, n1, ub, zb, rb, cap,
           w_sem, rest_sem, first_sem, x_sem, send_sem, recv_sem, y_sem):
    videos, frames, pairs, _, per_dev, width = x_hbm.shape
    rows = pairs * 2 * per_dev
    steps = videos * frames
    half = rows // 2
    groups = per_dev // SUB
    chunks = groups // 2
    me = lax.axis_index("sp")
    peers = n_sp - 1

    barrier = pltpu.get_barrier_semaphore()

    @pl.loop(1, n_sp)
    def _(k):
        pl.semaphore_signal(barrier, inc=1, device_id={"sp": lax.rem(me + k, n_sp)}, device_id_type=MESH)

    weights = ((wout_hbm, wout), (wup_hbm, wup), (wdown_hbm, wdown))

    def load(i, layer):
        return pltpu.make_async_copy(weights[i][0].at[layer], weights[i][1], w_sem.at[i])

    def load_x(s, m):
        return pltpu.make_async_copy(
            x_hbm.at[s // frames, s % frames, :, m], xb.at[s % 2, m], x_sem.at[s % 2, m])

    tiles = pl.cdiv(3 * width, TILE)
    first = column_tiles(head_windows(heads, head_dim), 0, (0, 1, 2), width)
    rest = [t for t in range(tiles) if t not in first]
    extra = [t for t in range(width // TILE) if t not in first]

    def load_tile(t, layer):
        cols = columns(t, width)
        home, sem = (wfirst.at[first.index(t)], first_sem) if t in first else (wrest.at[rest.index(t)], rest_sem)
        size = cols.stop - cols.start
        return pltpu.make_async_copy(
            wqkv_hbm.at[layer, :, pl.ds(cols.start, size)], home.at[:, pl.ds(0, size)],
            sem.at[(first if t in first else rest).index(t)])

    def w_of(t):
        cols = columns(t, width)
        size = cols.stop - cols.start
        return wfirst[first.index(t)] if t in first else wrest[rest.index(t), :, :size]

    def norm_next(layer, s, m):
        norms = norm_ref[layer].astype(f32)
        n1[m] = layer_norm(xb[s % 2, m].reshape(half, width), norms[0:1], norms[1:2])

    def project_first(m):
        for t in first:
            project_piece(n1, w_of(t), qk, vt, t, m)

    for m in range(2):
        load_x(0, m).start()
    for t in first + rest:
        load_tile(t, 0).start()
    for i in range(3):
        load(i, 0).start()
    for m in range(2):
        load_x(1, m).start()

    def frame_rows(s):
        return pl.ds(pl.multiple_of((me * frames + s % frames) * SUB, SUB), SUB)

    def send(s, m, pair):
        return pltpu.make_async_remote_copy(
            src_ref=zb.at[s, pl.ds((m * pairs + pair) * groups, groups)],
            dst_ref=rb.at[s // frames, :, frame_rows(s), :],
            send_sem=send_sem.at[s], recv_sem=recv_sem.at[s // frames],
            device_id={"sp": 2 * pair + m}, device_id_type=MESH)

    def result_rows(c, m):
        return pl.ds(pl.multiple_of(me * per_dev + (c % chunks * 2 + m) * SUB, SUB), SUB)

    def give(c, m, j):
        return pltpu.make_async_remote_copy(
            src_ref=zb.at[c, pl.ds((m * n_sp + j) * frames, frames)],
            dst_ref=y_ref.at[c // chunks, :, result_rows(c, m), :],
            send_sem=send_sem.at[c], recv_sem=y_sem, device_id={"sp": j}, device_id_type=MESH)

    def pair_at(i):
        turn = (i + 1) // 2 * (1 - 2 * (i % 2))
        return lax.rem(me // 2 + pairs // 2 + turn + pairs, pairs)

    def wait_sent(slot):
        sent = zb.at[slot, pl.ds(0, peers * groups)]
        pltpu.make_async_copy(sent, sent, send_sem.at[slot]).wait()

    for m in range(2):
        load_x(0, m).wait()
    for t in first:
        load_tile(t, 0).wait()
    for m in range(2):
        norm_next(0, 0, m)
        project_first(m)
    for t in rest:
        load_tile(t, 0).wait()

    @pl.loop(0, 2 * steps)
    def _(s):
        spatial = s < steps
        temporal = s >= steps
        layer = s // steps
        slot = s % steps
        xs = xb.at[s % 2]
        attention = functools.partial(attend, n1, w_of, qk, vt, ab, heads, head_dim)
        there = {(t, r) for t in first for r in range(2)}

        def out(m):
            hb[...] = residual(xs[m].reshape(half, width), project(ab[...], wout[...]))

        def norm():
            norms = norm_ref[layer].astype(f32)
            ab[...] = layer_norm(hb[...], norms[2:3], norms[3:4])

        def up():
            ub[...] = gelu(project(ab[...], wup[...]))

        def down(m):
            z = residual(hb[...], project(ub[...], wdown[...]))
            zb[slot, m * (half // SUB):(m + 1) * (half // SUB)] = z.reshape(half // SUB, SUB, width)

        def deliver(m):
            @pl.when(spatial)
            def _():
                @pl.loop(0, pairs)
                def _(i):
                    pair = pair_at(i)

                    @pl.when(2 * pair + m != me)
                    def _():
                        send(s, m, pair).start()

                @pl.when(m == me % 2)
                def _():
                    for g in range(groups):
                        rb[s // frames, g, frame_rows(s), :] = zb[s, (m * pairs + me // 2) * groups + g]

            @pl.when(temporal)
            def _():
                @pl.loop(0, pairs - 1)
                def _(i):
                    for core in range(2):
                        give(slot, m, 2 * pair_at(i) + core).start()
                give(slot, m, me + 1 - 2 * (me % 2)).start()
                for f in range(frames):
                    y_ref[slot // chunks, f, result_rows(slot, m), :] = zb[slot, (m * n_sp + me) * frames + f]

        @pl.when(spatial)
        def _():
            attention(0, (0, 1), there, 3, 2, None)

        @pl.when(temporal)
        def _():
            attention(0, (0,), there, 3, 3, cap)

        for i in range(2):
            load(i, layer).wait()

        @pl.when(slot == 0)
        def _():
            load(2, layer).wait()

        @pl.when(temporal)
        def _():
            wait_sent(slot)

        out(0)
        for t in extra:
            project_piece(n1, w_of(t), qk, vt, t, 1)
        norm()
        up()
        down(0)

        @pl.when(s == 0)
        def _():
            pl.semaphore_wait(barrier, peers)

        deliver(0)

        @pl.when(spatial)
        def _():
            attention(1, (0, 1), {(t, r) for t in range(tiles) for r in range(2)}, 5, 3, None)

        @pl.when(temporal)
        def _():
            attention(1, (1,), there | {(t, 1) for t in extra}, 4, 3, cap)

        @pl.when(s == steps - 1)
        def _():
            for t in rest:
                load_tile(t, 1).start()
            for t in first:
                load_tile(t, 1).wait()

        @pl.when(s + 1 < steps)
        def _():
            for m in range(2):
                load_x(s + 1, m).wait()

        @pl.when(jnp.logical_and(s + 1 >= steps, s + 1 < 2 * steps))
        def _():
            c = s + 1 - steps

            @pl.when(c % chunks == 0)
            def _():
                v = c // chunks
                got = rb.at[v, :, pl.ds(0, peers * frames * SUB), :]
                pltpu.make_async_copy(got, got, recv_sem.at[v]).wait()
                shift = SUB.bit_length() - 1
                limit = len_ref[v]
                for r in range(0, half, LANES):
                    ki = lax.broadcasted_iota(jnp.int32, (LANES, half), 0) + r
                    qi = lax.broadcasted_iota(jnp.int32, (LANES, half), 1)
                    kt = lax.shift_right_logical(ki, shift)
                    ok = ((qi & (SUB - 1)) == (ki & (SUB - 1))) & (kt <= lax.shift_right_logical(qi, shift)) & (kt < limit)
                    cap[r:r + LANES, :] = jnp.where(ok, OPEN, MASKED)

            for m in range(2):
                xb[(s + 1) % 2, m] = rb[c // chunks, c % chunks * 2 + m].reshape(pairs, per_dev, width)

        after = jnp.minimum((s + 1) // steps, 1)
        norm_next(after, s + 1, 0)
        out(1)
        load(0, after).start()
        project_first(0)
        norm()
        up()
        load(1, after).start()
        norm_next(after, s + 1, 1)
        project_first(1)
        down(1)
        deliver(1)

        @pl.when(s == steps - 1)
        def _():
            for t in rest:
                load_tile(t, 1).wait()
            load(2, 1).start()

        @pl.when(s == steps - 2)
        def _():
            for t in first:
                load_tile(t, 1).start()

        @pl.when(s + 2 < steps)
        def _():
            for m in range(2):
                load_x(s + 2, m).start()

    for i in range(2):
        load(i, 1).wait()
    for slot in range(steps):
        wait_sent(slot)
    got = y_ref.at[:, :, pl.ds(0, peers * per_dev), :]
    pltpu.make_async_copy(got, got, y_sem).wait()


def solution(mesh):
    act_spec = P('data', 'sp', None, None)
    n_sp = mesh.shape['sp']

    def local_step(latents, valid_len, norm_w, w_qkv, w_out, w_up, w_down):
        videos, frames, rows, width = latents.shape
        heads, head_dim = w_out.shape[1:3]
        hidden = w_up.shape[2]
        tokens = videos * frames * rows
        half = rows // 2
        any_spec = pl.BlockSpec(memory_space=pl.ANY)
        dma = pltpu.SemaphoreType.DMA
        steps = videos * frames
        firsts = len(column_tiles(head_windows(heads, head_dim), 0, (0, 1, 2), width))
        rests = pl.cdiv(3 * width, TILE) - firsts
        return pl.pallas_call(
            functools.partial(kernel, n_sp, heads, head_dim),
            out_shape=pltpu.VMEM(latents.shape, bf16),
            in_specs=[any_spec, pl.BlockSpec(memory_space=pltpu.SMEM), pl.BlockSpec(memory_space=pltpu.VMEM)] + [any_spec] * 4,
            out_specs=pl.BlockSpec(memory_space=pltpu.VMEM),
            scratch_shapes=[
                pltpu.VMEM((rests, width, TILE), bf16), pltpu.VMEM((firsts, width, TILE), bf16),
                pltpu.VMEM((width, width), bf16),
                pltpu.VMEM((width, hidden), bf16), pltpu.VMEM((hidden, width), bf16),
                pltpu.VMEM((2, 2, n_sp // 2, rows // n_sp, width), bf16), pltpu.VMEM((2, half, 2 * width), bf16),
                pltpu.VMEM((width, rows), bf16),
                pltpu.VMEM((half, width), bf16), pltpu.VMEM((half, width), bf16),
                pltpu.VMEM((2, half, width), bf16),
                pltpu.VMEM((half, hidden), bf16), pltpu.VMEM((steps, rows // SUB, SUB, width), bf16),
                pltpu.VMEM((videos, rows // n_sp // SUB, n_sp * frames * SUB, width), bf16), pltpu.VMEM((half, half), f32),
                dma((3,)), dma((rests,)), dma((firsts,)), dma((2, 2)), dma((steps,)), dma((videos,)), dma,
            ],
            compiler_params=pltpu.CompilerParams(collective_id=0, has_side_effects=True, vmem_limit_bytes=62_000_000),
            cost_estimate=pl.CostEstimate(
                flops=2 * 2 * tokens * width * (4 * width + 2 * hidden), bytes_accessed=70_000_000, transcendentals=0),
            name="dit",
        )(latents.reshape(videos, frames, n_sp // 2, 2, rows // n_sp, width), valid_len, norm_w, w_qkv, w_out.reshape(2, width, width), w_up, w_down)

    return jax.shard_map(local_step, mesh=mesh, in_specs=(act_spec, P('data'), P(), P(), P(), P(), P()), out_specs=act_spec, check_vma=False)
```

```python
import functools
import math

import jax
import jax.numpy as jnp
from jax import lax
from jax.experimental import pallas as pl
from jax.experimental.pallas import tpu as pltpu
from jax.sharding import PartitionSpec as P

LN_EPS = 1e-6
MASKED = -1e30
OPEN = 3e38
LANES = 128
TILE = 256
SUB = 8
PACK = 16
f32, bf16 = jnp.float32, jnp.bfloat16
MESH = pl.DeviceIdType.MESH


def layer_norm(tokens, gain, shift):
    values = tokens.astype(f32)
    inv_width = 1.0 / values.shape[-1]
    centered = values - jnp.sum(values, -1, keepdims=True) * inv_width
    variance = jnp.sum(centered * centered, -1, keepdims=True) * inv_width
    return (centered * lax.rsqrt(variance + LN_EPS) * gain + shift).astype(bf16)


def project(a, b):
    return jnp.dot(a, b, preferred_element_type=f32).astype(bf16)


def residual(base, delta):
    return (base.astype(f32) + delta.astype(f32)).astype(bf16)


def gelu(u):
    x = u.astype(f32)
    c = math.sqrt(2.0 / math.pi)
    half = 0.5 * x
    return (half + half * jnp.tanh(x * (x * x * (c * 0.044715) + c))).astype(bf16)


def head_windows(heads, head_dim):
    out = []
    for h in range(heads):
        lo = h * head_dim
        base = lo // LANES * LANES
        out.append((lo, base, LANES if lo + head_dim <= base + LANES else 2 * LANES))
    return out


def column_tiles(wins, h, parts, width):
    _, base, w = wins[h]
    spans = [(p * width + base, p * width + base + w - 1) for p in parts]
    return list(dict.fromkeys(t for lo, hi in spans for t in range(lo // TILE, hi // TILE + 1)))


def columns(t, width):
    return slice(t * TILE, min((t + 1) * TILE, 3 * width))


def attend(nb, w_of, qk, vt, a_ref, heads, head_dim, mine, key_halves, made, look, lead, cap_ref):
    _, half, width = nb.shape
    scale = head_dim ** -0.5 * math.log2(math.e)
    wins = head_windows(heads, head_dim)
    made = set(made)
    key_rows = slice(key_halves[0] * half, (key_halves[-1] + 1) * half)

    def pieces(h, parts):
        return [(t, r) for p in parts for t in column_tiles(wins, h, (p,), width) for r in ((mine,) if p == 0 else key_halves)]

    def make(t, r):
        if (t, r) not in made:
            made.add((t, r))
            project_piece(nb, w_of(t), qk, vt, t, r)

    def keys(cols):
        return jnp.concatenate([qk[r, :, cols] for r in key_halves], axis=0)

    def scores(h):
        for u in pieces(h, (0, 1)):
            make(*u)
        lo, base, w_ = wins[h]
        lane = lax.broadcasted_iota(jnp.int32, (1, w_), 1) + base
        own = jnp.where((lane >= lo) & (lane < lo + head_dim), 1.0, 0.0).astype(bf16)
        q = qk[mine, :, base:base + w_] * own
        k = keys(slice(width + base, width + base + w_))
        return lax.dot_general(k, q, (((1,), (1,)), ((), ())), preferred_element_type=f32)

    due = []
    for h in range(heads):
        for p, step in ((0, h - look), (1, h - look), (2, h)):
            due += [(max(step, -1), u) for u in pieces(h, (p,))]
    ready = {h: scores(h) for h in range(look)}
    done, parts = 0, []
    for h in range(heads):
        for step, u in sorted(due, key=lambda d: d[0]):
            if step <= h + lead:
                make(*u)
        if h + look < heads:
            ready[h + look] = scores(h + look)
        s = ready.pop(h)
        if cap_ref is not None:
            s = jnp.minimum(s, cap_ref[...])
        e = jnp.exp2((s - jnp.max(s, 0, keepdims=True)) * scale)
        p = (e * (1.0 / jnp.sum(e, 0, keepdims=True))).astype(bf16)
        lo = h * head_dim
        r0, r1 = lo // PACK * PACK, pl.cdiv(lo + head_dim, PACK) * PACK
        o = jnp.dot(vt[r0:r1, key_rows], p, preferred_element_type=f32)
        parts.append((lo, o[lo - r0:lo - r0 + head_dim, :]))
        while (done + 1) * LANES <= lo + head_dim:
            g0, g1 = done * LANES, (done + 1) * LANES
            rows = [x[max(g0 - l, 0):min(g1 - l, head_dim), :] for l, x in parts if l < g1]
            a_ref[:, g0:g1] = jnp.concatenate(rows, axis=0).astype(bf16).T
            parts = [(l, x) for l, x in parts if l + head_dim > g1]
            done += 1


def project_piece(nb, w, qk, vt, t, r):
    half, width = nb.shape[1:]
    piece = project(nb[r], w)
    cols = columns(t, width)
    if cols.start < 2 * width:
        qk[r, :, cols] = piece
    else:
        vt[cols.start - 2 * width:cols.stop - 2 * width, r * half:(r + 1) * half] = piece.T


def kernel(n_sp, heads, head_dim, x_hbm, len_ref, norm_ref, wqkv_hbm, wout_hbm, wup_hbm, wdown_hbm, y_ref,
           wrest, wfirst, wout, wup, wdown, xb, qk, vt, ab, hb, n1, ub, zb, rb, cap,
           w_sem, rest_sem, first_sem, x_sem, send_sem, recv_sem, y_sem):
    videos, frames, pairs, _, per_dev, width = x_hbm.shape
    rows = pairs * 2 * per_dev
    steps = videos * frames
    half = rows // 2
    groups = per_dev // SUB
    chunks = groups // 2
    me = lax.axis_index("sp")
    peers = n_sp - 1

    barrier = pltpu.get_barrier_semaphore()

    @pl.loop(1, n_sp)
    def _(k):
        pl.semaphore_signal(barrier, inc=1, device_id={"sp": lax.rem(me + k, n_sp)}, device_id_type=MESH)

    weights = ((wout_hbm, wout), (wup_hbm, wup), (wdown_hbm, wdown))

    def load(i, layer):
        return pltpu.make_async_copy(weights[i][0].at[layer], weights[i][1], w_sem.at[i])

    def load_x(s, m):
        return pltpu.make_async_copy(
            x_hbm.at[s // frames, s % frames, :, m], xb.at[s % 2, m], x_sem.at[s % 2, m])

    tiles = pl.cdiv(3 * width, TILE)
    first = column_tiles(head_windows(heads, head_dim), 0, (0, 1, 2), width)
    rest = [t for t in range(tiles) if t not in first]
    extra = [t for t in range(width // TILE) if t not in first]

    def load_tile(t, layer):
        cols = columns(t, width)
        home, sem = (wfirst.at[first.index(t)], first_sem) if t in first else (wrest.at[rest.index(t)], rest_sem)
        size = cols.stop - cols.start
        return pltpu.make_async_copy(
            wqkv_hbm.at[layer, :, pl.ds(cols.start, size)], home.at[:, pl.ds(0, size)],
            sem.at[(first if t in first else rest).index(t)])

    def w_of(t):
        cols = columns(t, width)
        size = cols.stop - cols.start
        return wfirst[first.index(t)] if t in first else wrest[rest.index(t), :, :size]

    def norm_next(layer, s, m):
        norms = norm_ref[layer].astype(f32)
        n1[m] = layer_norm(xb[s % 2, m].reshape(half, width), norms[0:1], norms[1:2])

    def project_first(m):
        for t in first:
            project_piece(n1, w_of(t), qk, vt, t, m)

    for m in range(2):
        load_x(0, m).start()
    for t in first + rest:
        load_tile(t, 0).start()

    def frame_rows(s):
        return pl.ds(pl.multiple_of((me * frames + s % frames) * SUB, SUB), SUB)

    def send(s, m, pair):
        return pltpu.make_async_remote_copy(
            src_ref=zb.at[s, pl.ds((m * pairs + pair) * groups, groups)],
            dst_ref=rb.at[s // frames, :, frame_rows(s), :],
            send_sem=send_sem.at[s], recv_sem=recv_sem.at[s // frames],
            device_id={"sp": 2 * pair + m}, device_id_type=MESH)

    def result_rows(c, m):
        return pl.ds(pl.multiple_of(me * per_dev + (c % chunks * 2 + m) * SUB, SUB), SUB)

    def give(c, m, j):
        return pltpu.make_async_remote_copy(
            src_ref=zb.at[c, pl.ds((m * n_sp + j) * frames, frames)],
            dst_ref=y_ref.at[c // chunks, :, result_rows(c, m), :],
            send_sem=send_sem.at[c], recv_sem=y_sem, device_id={"sp": j}, device_id_type=MESH)

    def pair_at(i):
        turn = (i + 1) // 2 * (1 - 2 * (i % 2))
        return lax.rem(me // 2 + pairs // 2 + turn + pairs, pairs)

    def wait_sent(slot):
        sent = zb.at[slot, pl.ds(0, peers * groups)]
        pltpu.make_async_copy(sent, sent, send_sem.at[slot]).wait()

    for m in range(2):
        load_x(0, m).wait()
    for t in first:
        load_tile(t, 0).wait()
    for i in range(3):
        load(i, 0).start()
    for m in range(2):
        load_x(1, m).start()
    for m in range(2):
        norm_next(0, 0, m)
        project_first(m)
    for t in rest:
        load_tile(t, 0).wait()

    @pl.loop(0, 2 * steps)
    def _(s):
        spatial = s < steps
        temporal = s >= steps
        layer = s // steps
        slot = s % steps
        xs = xb.at[s % 2]
        attention = functools.partial(attend, n1, w_of, qk, vt, ab, heads, head_dim)
        there = {(t, r) for t in first for r in range(2)}

        def out(m):
            hb[...] = residual(xs[m].reshape(half, width), project(ab[...], wout[...]))

        def norm():
            norms = norm_ref[layer].astype(f32)
            ab[...] = layer_norm(hb[...], norms[2:3], norms[3:4])

        def up():
            ub[...] = gelu(project(ab[...], wup[...]))

        def down(m):
            z = residual(hb[...], project(ub[...], wdown[...]))
            zb[slot, m * (half // SUB):(m + 1) * (half // SUB)] = z.reshape(half // SUB, SUB, width)

        def deliver(m):
            @pl.when(spatial)
            def _():
                @pl.loop(0, pairs)
                def _(i):
                    pair = pair_at(i)

                    @pl.when(2 * pair + m != me)
                    def _():
                        send(s, m, pair).start()

                @pl.when(m == me % 2)
                def _():
                    for g in range(groups):
                        rb[s // frames, g, frame_rows(s), :] = zb[s, (m * pairs + me // 2) * groups + g]

            @pl.when(temporal)
            def _():
                @pl.loop(0, pairs - 1)
                def _(i):
                    for core in range(2):
                        give(slot, m, 2 * pair_at(i) + core).start()
                give(slot, m, me + 1 - 2 * (me % 2)).start()
                for f in range(frames):
                    y_ref[slot // chunks, f, result_rows(slot, m), :] = zb[slot, (m * n_sp + me) * frames + f]

        @pl.when(spatial)
        def _():
            attention(0, (0, 1), there, 3, 2, None)

        @pl.when(temporal)
        def _():
            attention(0, (0,), there, 3, 3, cap)

        for i in range(2):
            load(i, layer).wait()

        @pl.when(slot == 0)
        def _():
            load(2, layer).wait()

        @pl.when(temporal)
        def _():
            wait_sent(slot)

        out(0)
        for t in extra:
            project_piece(n1, w_of(t), qk, vt, t, 1)
        norm()
        up()
        down(0)

        @pl.when(s == 0)
        def _():
            pl.semaphore_wait(barrier, peers)

        deliver(0)

        @pl.when(spatial)
        def _():
            attention(1, (0, 1), {(t, r) for t in range(tiles) for r in range(2)}, 5, 3, None)

        @pl.when(temporal)
        def _():
            attention(1, (1,), there | {(t, 1) for t in extra}, 4, 3, cap)

        @pl.when(s == steps - 1)
        def _():
            for t in rest:
                load_tile(t, 1).start()
            for t in first:
                load_tile(t, 1).wait()

        @pl.when(s + 1 < steps)
        def _():
            for m in range(2):
                load_x(s + 1, m).wait()

        @pl.when(jnp.logical_and(s + 1 >= steps, s + 1 < 2 * steps))
        def _():
            c = s + 1 - steps

            @pl.when(c % chunks == 0)
            def _():
                v = c // chunks
                got = rb.at[v, :, pl.ds(0, peers * frames * SUB), :]
                pltpu.make_async_copy(got, got, recv_sem.at[v]).wait()
                shift = SUB.bit_length() - 1
                limit = len_ref[v]
                for r in range(0, half, LANES):
                    ki = lax.broadcasted_iota(jnp.int32, (LANES, half), 0) + r
                    qi = lax.broadcasted_iota(jnp.int32, (LANES, half), 1)
                    kt = lax.shift_right_logical(ki, shift)
                    ok = ((qi & (SUB - 1)) == (ki & (SUB - 1))) & (kt <= lax.shift_right_logical(qi, shift)) & (kt < limit)
                    cap[r:r + LANES, :] = jnp.where(ok, OPEN, MASKED)

            for m in range(2):
                xb[(s + 1) % 2, m] = rb[c // chunks, c % chunks * 2 + m].reshape(pairs, per_dev, width)

        after = jnp.minimum((s + 1) // steps, 1)
        norm_next(after, s + 1, 0)
        out(1)
        load(0, after).start()
        project_first(0)
        norm()
        up()
        load(1, after).start()
        norm_next(after, s + 1, 1)
        project_first(1)
        down(1)
        deliver(1)

        @pl.when(s == steps - 1)
        def _():
            for t in rest:
                load_tile(t, 1).wait()
            load(2, 1).start()

        @pl.when(s == steps - 2)
        def _():
            for t in first:
                load_tile(t, 1).start()

        @pl.when(s + 2 < steps)
        def _():
            for m in range(2):
                load_x(s + 2, m).start()

    for i in range(2):
        load(i, 1).wait()
    for slot in range(steps):
        wait_sent(slot)
    got = y_ref.at[:, :, pl.ds(0, peers * per_dev), :]
    pltpu.make_async_copy(got, got, y_sem).wait()


def solution(mesh):
    act_spec = P('data', 'sp', None, None)
    n_sp = mesh.shape['sp']

    def local_step(latents, valid_len, norm_w, w_qkv, w_out, w_up, w_down):
        videos, frames, rows, width = latents.shape
        heads, head_dim = w_out.shape[1:3]
        hidden = w_up.shape[2]
        tokens = videos * frames * rows
        half = rows // 2
        any_spec = pl.BlockSpec(memory_space=pl.ANY)
        dma = pltpu.SemaphoreType.DMA
        steps = videos * frames
        firsts = len(column_tiles(head_windows(heads, head_dim), 0, (0, 1, 2), width))
        rests = pl.cdiv(3 * width, TILE) - firsts
        return pl.pallas_call(
            functools.partial(kernel, n_sp, heads, head_dim),
            out_shape=pltpu.VMEM(latents.shape, bf16),
            in_specs=[any_spec, pl.BlockSpec(memory_space=pltpu.SMEM), pl.BlockSpec(memory_space=pltpu.VMEM)] + [any_spec] * 4,
            out_specs=pl.BlockSpec(memory_space=pltpu.VMEM),
            scratch_shapes=[
                pltpu.VMEM((rests, width, TILE), bf16), pltpu.VMEM((firsts, width, TILE), bf16),
                pltpu.VMEM((width, width), bf16),
                pltpu.VMEM((width, hidden), bf16), pltpu.VMEM((hidden, width), bf16),
                pltpu.VMEM((2, 2, n_sp // 2, rows // n_sp, width), bf16), pltpu.VMEM((2, half, 2 * width), bf16),
                pltpu.VMEM((width, rows), bf16),
                pltpu.VMEM((half, width), bf16), pltpu.VMEM((half, width), bf16),
                pltpu.VMEM((2, half, width), bf16),
                pltpu.VMEM((half, hidden), bf16), pltpu.VMEM((steps, rows // SUB, SUB, width), bf16),
                pltpu.VMEM((videos, rows // n_sp // SUB, n_sp * frames * SUB, width), bf16), pltpu.VMEM((half, half), f32),
                dma((3,)), dma((rests,)), dma((firsts,)), dma((2, 2)), dma((steps,)), dma((videos,)), dma,
            ],
            compiler_params=pltpu.CompilerParams(collective_id=0, has_side_effects=True, vmem_limit_bytes=62_000_000),
            cost_estimate=pl.CostEstimate(
                flops=2 * 2 * tokens * width * (4 * width + 2 * hidden), bytes_accessed=70_000_000, transcendentals=0),
            name="dit",
        )(latents.reshape(videos, frames, n_sp // 2, 2, rows // n_sp, width), valid_len, norm_w, w_qkv, w_out.reshape(2, width, width), w_up, w_down)

    return jax.shard_map(local_step, mesh=mesh, in_specs=(act_spec, P('data'), P(), P(), P(), P(), P()), out_specs=act_spec, check_vma=False)
```

```python
import functools
import math

import jax
import jax.numpy as jnp
from jax import lax
from jax.experimental import pallas as pl
from jax.experimental.pallas import tpu as pltpu
from jax.sharding import PartitionSpec as P

LN_EPS = 1e-6
MASKED = -1e30
OPEN = 3e38
LANES = 128
TILE = 256
SUB = 8
PACK = 16
f32, bf16 = jnp.float32, jnp.bfloat16
MESH = pl.DeviceIdType.MESH


def layer_norm(tokens, gain, shift):
    values = tokens.astype(f32)
    inv_width = 1.0 / values.shape[-1]
    centered = values - jnp.sum(values, -1, keepdims=True) * inv_width
    variance = jnp.sum(centered * centered, -1, keepdims=True) * inv_width
    return (centered * lax.rsqrt(variance + LN_EPS) * gain + shift).astype(bf16)


def project(a, b):
    return jnp.dot(a, b, preferred_element_type=f32).astype(bf16)


def residual(base, delta):
    return (base.astype(f32) + delta.astype(f32)).astype(bf16)


def gelu(u):
    x = u.astype(f32)
    c = math.sqrt(2.0 / math.pi)
    half = 0.5 * x
    return (half + half * jnp.tanh(x * (x * x * (c * 0.044715) + c))).astype(bf16)


def head_windows(heads, head_dim):
    out = []
    for h in range(heads):
        lo = h * head_dim
        base = lo // LANES * LANES
        out.append((lo, base, LANES if lo + head_dim <= base + LANES else 2 * LANES))
    return out


def column_tiles(wins, h, parts, width):
    _, base, w = wins[h]
    spans = [(p * width + base, p * width + base + w - 1) for p in parts]
    return list(dict.fromkeys(t for lo, hi in spans for t in range(lo // TILE, hi // TILE + 1)))


def columns(t, width):
    return slice(t * TILE, min((t + 1) * TILE, 3 * width))


def attend(nb, w_of, qk, vt, a_ref, heads, head_dim, mine, key_halves, made, look, lead, cap_ref):
    _, half, width = nb.shape
    scale = head_dim ** -0.5 * math.log2(math.e)
    wins = head_windows(heads, head_dim)
    made = set(made)
    key_rows = slice(key_halves[0] * half, (key_halves[-1] + 1) * half)

    def pieces(h, parts):
        return [(t, r) for p in parts for t in column_tiles(wins, h, (p,), width) for r in ((mine,) if p == 0 else key_halves)]

    def make(t, r):
        if (t, r) not in made:
            made.add((t, r))
            project_piece(nb, w_of(t), qk, vt, t, r)

    def keys(cols):
        return jnp.concatenate([qk[r, :, cols] for r in key_halves], axis=0)

    def scores(h):
        for u in pieces(h, (0, 1)):
            make(*u)
        lo, base, w_ = wins[h]
        lane = lax.broadcasted_iota(jnp.int32, (1, w_), 1) + base
        own = jnp.where((lane >= lo) & (lane < lo + head_dim), 1.0, 0.0).astype(bf16)
        q = qk[mine, :, base:base + w_] * own
        k = keys(slice(width + base, width + base + w_))
        return lax.dot_general(k, q, (((1,), (1,)), ((), ())), preferred_element_type=f32)

    due = []
    for h in range(heads):
        for p, step in ((0, h - look), (1, h - look), (2, h)):
            due += [(max(step, -1), u) for u in pieces(h, (p,))]
    ready = {h: scores(h) for h in range(look)}
    done, parts = 0, []
    for h in range(heads):
        for step, u in sorted(due, key=lambda d: d[0]):
            if step <= h + lead:
                make(*u)
        if h + look < heads:
            ready[h + look] = scores(h + look)
        s = ready.pop(h)
        if cap_ref is not None:
            s = jnp.minimum(s, cap_ref[...])
        e = jnp.exp2((s - jnp.max(s, 0, keepdims=True)) * scale)
        p = (e * (1.0 / jnp.sum(e, 0, keepdims=True))).astype(bf16)
        lo = h * head_dim
        r0, r1 = lo // PACK * PACK, pl.cdiv(lo + head_dim, PACK) * PACK
        o = jnp.dot(vt[r0:r1, key_rows], p, preferred_element_type=f32)
        parts.append((lo, o[lo - r0:lo - r0 + head_dim, :]))
        while (done + 1) * LANES <= lo + head_dim:
            g0, g1 = done * LANES, (done + 1) * LANES
            rows = [x[max(g0 - l, 0):min(g1 - l, head_dim), :] for l, x in parts if l < g1]
            a_ref[:, g0:g1] = jnp.concatenate(rows, axis=0).astype(bf16).T
            parts = [(l, x) for l, x in parts if l + head_dim > g1]
            done += 1


def project_piece(nb, w, qk, vt, t, r):
    half, width = nb.shape[1:]
    piece = project(nb[r], w)
    cols = columns(t, width)
    if cols.start < 2 * width:
        qk[r, :, cols] = piece
    else:
        vt[cols.start - 2 * width:cols.stop - 2 * width, r * half:(r + 1) * half] = piece.T


def kernel(n_sp, heads, head_dim, x_hbm, len_ref, norm_ref, wqkv_hbm, wout_hbm, wup_hbm, wdown_hbm, y_ref,
           wrest, wfirst, wout, wup, wdown, xb, qk, vt, ab, hb, n1, ub, zb, rb, cap,
           w_sem, rest_sem, first_sem, x_sem, send_sem, recv_sem, y_sem):
    videos, frames, pairs, _, per_dev, width = x_hbm.shape
    rows = pairs * 2 * per_dev
    steps = videos * frames
    half = rows // 2
    groups = per_dev // SUB
    chunks = groups // 2
    me = lax.axis_index("sp")
    peers = n_sp - 1

    barrier = pltpu.get_barrier_semaphore()

    @pl.loop(1, n_sp)
    def _(k):
        pl.semaphore_signal(barrier, inc=1, device_id={"sp": lax.rem(me + k, n_sp)}, device_id_type=MESH)

    weights = ((wout_hbm, wout), (wup_hbm, wup), (wdown_hbm, wdown))

    def load(i, layer):
        return pltpu.make_async_copy(weights[i][0].at[layer], weights[i][1], w_sem.at[i])

    def load_x(s, m):
        return pltpu.make_async_copy(
            x_hbm.at[s // frames, s % frames, :, m], xb.at[s % 2, m], x_sem.at[s % 2, m])

    tiles = pl.cdiv(3 * width, TILE)
    first = column_tiles(head_windows(heads, head_dim), 0, (0, 1, 2), width)
    rest = [t for t in range(tiles) if t not in first]
    extra = [t for t in range(width // TILE) if t not in first]

    def load_tile(t, layer):
        cols = columns(t, width)
        home, sem = (wfirst.at[first.index(t)], first_sem) if t in first else (wrest.at[rest.index(t)], rest_sem)
        size = cols.stop - cols.start
        return pltpu.make_async_copy(
            wqkv_hbm.at[layer, :, pl.ds(cols.start, size)], home.at[:, pl.ds(0, size)],
            sem.at[(first if t in first else rest).index(t)])

    def w_of(t):
        cols = columns(t, width)
        size = cols.stop - cols.start
        return wfirst[first.index(t)] if t in first else wrest[rest.index(t), :, :size]

    def norm_next(layer, s, m):
        norms = norm_ref[layer].astype(f32)
        n1[m] = layer_norm(xb[s % 2, m].reshape(half, width), norms[0:1], norms[1:2])

    def project_first(m):
        for t in first:
            project_piece(n1, w_of(t), qk, vt, t, m)

    for m in range(2):
        load_x(0, m).start()
    for t in first + rest:
        load_tile(t, 0).start()

    def frame_rows(s):
        return pl.ds(pl.multiple_of((me * frames + s % frames) * SUB, SUB), SUB)

    def send(s, m, pair):
        return pltpu.make_async_remote_copy(
            src_ref=zb.at[s, pl.ds((m * pairs + pair) * groups, groups)],
            dst_ref=rb.at[s // frames, :, frame_rows(s), :],
            send_sem=send_sem.at[s], recv_sem=recv_sem.at[s // frames],
            device_id={"sp": 2 * pair + m}, device_id_type=MESH)

    def result_rows(c, m):
        return pl.ds(pl.multiple_of(me * per_dev + (c % chunks * 2 + m) * SUB, SUB), SUB)

    def give(c, m, j):
        return pltpu.make_async_remote_copy(
            src_ref=zb.at[c, pl.ds((m * n_sp + j) * frames, frames)],
            dst_ref=y_ref.at[c // chunks, :, result_rows(c, m), :],
            send_sem=send_sem.at[c], recv_sem=y_sem, device_id={"sp": j}, device_id_type=MESH)

    mine = me // 2
    turns = [(pairs // 2 + (i + 1) // 2 * (1 - 2 * (i % 2))) % pairs for i in range(pairs - 1)]

    def wait_sent(slot):
        sent = zb.at[slot, pl.ds(0, peers * groups)]
        pltpu.make_async_copy(sent, sent, send_sem.at[slot]).wait()

    for m in range(2):
        load_x(0, m).wait()
    for t in first:
        load_tile(t, 0).wait()
    for i in range(3):
        load(i, 0).start()
    for m in range(2):
        load_x(1, m).start()
    for m in range(2):
        norm_next(0, 0, m)
        project_first(m)
    for t in rest:
        load_tile(t, 0).wait()

    @pl.loop(0, 2 * steps)
    def _(s):
        spatial = s < steps
        temporal = s >= steps
        layer = s // steps
        slot = s % steps
        xs = xb.at[s % 2]
        attention = functools.partial(attend, n1, w_of, qk, vt, ab, heads, head_dim)
        there = {(t, r) for t in first for r in range(2)}

        def out(m):
            hb[...] = residual(xs[m].reshape(half, width), project(ab[...], wout[...]))

        def norm():
            norms = norm_ref[layer].astype(f32)
            ab[...] = layer_norm(hb[...], norms[2:3], norms[3:4])

        def up():
            ub[...] = gelu(project(ab[...], wup[...]))

        def down(m):
            z = residual(hb[...], project(ub[...], wdown[...]))
            zb[slot, m * (half // SUB):(m + 1) * (half // SUB)] = z.reshape(half // SUB, SUB, width)

        def keep_frame(m):
            @pl.when(m == me % 2)
            def _():
                for g in range(groups):
                    rb[s // frames, g, frame_rows(s), :] = zb[s, (m * pairs + mine) * groups + g]

            @pl.when(m != me % 2)
            def _():
                send(s, m, mine).start()

        def send_frame(m):
            for t in turns:
                send(s, m, lax.rem(mine + t, pairs)).start()

        def send_result(m):
            for t in turns:
                for core in range(2):
                    give(slot, m, 2 * lax.rem(mine + t, pairs) + core).start()
            give(slot, m, me + 1 - 2 * (me % 2)).start()
            for f in range(frames):
                y_ref[slot // chunks, f, result_rows(slot, m), :] = zb[slot, (m * n_sp + me) * frames + f]

        @pl.when(spatial)
        def _():
            attention(0, (0, 1), there, 3, 2, None)

        @pl.when(temporal)
        def _():
            attention(0, (0,), there, 3, 3, cap)

        for i in range(2):
            load(i, layer).wait()

        @pl.when(slot == 0)
        def _():
            load(2, layer).wait()

        @pl.when(temporal)
        def _():
            wait_sent(slot)

        out(0)
        for t in extra:
            project_piece(n1, w_of(t), qk, vt, t, 1)
        norm()
        up()
        down(0)

        @pl.when(s == 0)
        def _():
            pl.semaphore_wait(barrier, peers)

        @pl.when(spatial)
        def _():
            keep_frame(0)
            send_frame(0)
            attention(1, (0, 1), {(t, r) for t in range(tiles) for r in range(2)}, 5, 3, None)

        @pl.when(temporal)
        def _():
            send_result(0)
            attention(1, (1,), there | {(t, 1) for t in extra}, 4, 3, cap)

        @pl.when(s == steps - 1)
        def _():
            for t in rest:
                load_tile(t, 1).start()
            for t in first:
                load_tile(t, 1).wait()

        @pl.when(s + 1 < steps)
        def _():
            for m in range(2):
                load_x(s + 1, m).wait()

        @pl.when(jnp.logical_and(s + 1 >= steps, s + 1 < 2 * steps))
        def _():
            c = s + 1 - steps

            @pl.when(c % chunks == 0)
            def _():
                v = c // chunks
                got = rb.at[v, :, pl.ds(0, peers * frames * SUB), :]
                pltpu.make_async_copy(got, got, recv_sem.at[v]).wait()
                shift = SUB.bit_length() - 1
                limit = len_ref[v]
                for r in range(0, half, LANES):
                    ki = lax.broadcasted_iota(jnp.int32, (LANES, half), 0) + r
                    qi = lax.broadcasted_iota(jnp.int32, (LANES, half), 1)
                    kt = lax.shift_right_logical(ki, shift)
                    ok = ((qi & (SUB - 1)) == (ki & (SUB - 1))) & (kt <= lax.shift_right_logical(qi, shift)) & (kt < limit)
                    cap[r:r + LANES, :] = jnp.where(ok, OPEN, MASKED)

            for m in range(2):
                xb[(s + 1) % 2, m] = rb[c // chunks, c % chunks * 2 + m].reshape(pairs, per_dev, width)

        after = jnp.minimum((s + 1) // steps, 1)
        norm_next(after, s + 1, 0)
        out(1)
        load(0, after).start()
        project_first(0)
        norm()
        up()
        load(1, after).start()
        norm_next(after, s + 1, 1)
        project_first(1)
        down(1)

        @pl.when(spatial)
        def _():
            keep_frame(1)
            send_frame(1)

        @pl.when(temporal)
        def _():
            send_result(1)

        @pl.when(s == steps - 1)
        def _():
            for t in rest:
                load_tile(t, 1).wait()
            load(2, 1).start()

        @pl.when(s == steps - 2)
        def _():
            for t in first:
                load_tile(t, 1).start()

        @pl.when(s + 2 < steps)
        def _():
            for m in range(2):
                load_x(s + 2, m).start()

    for i in range(2):
        load(i, 1).wait()
    for slot in range(steps):
        wait_sent(slot)
    got = y_ref.at[:, :, pl.ds(0, peers * per_dev), :]
    pltpu.make_async_copy(got, got, y_sem).wait()


def solution(mesh):
    act_spec = P('data', 'sp', None, None)
    n_sp = mesh.shape['sp']

    def local_step(latents, valid_len, norm_w, w_qkv, w_out, w_up, w_down):
        videos, frames, rows, width = latents.shape
        heads, head_dim = w_out.shape[1:3]
        hidden = w_up.shape[2]
        tokens = videos * frames * rows
        half = rows // 2
        any_spec = pl.BlockSpec(memory_space=pl.ANY)
        dma = pltpu.SemaphoreType.DMA
        steps = videos * frames
        firsts = len(column_tiles(head_windows(heads, head_dim), 0, (0, 1, 2), width))
        rests = pl.cdiv(3 * width, TILE) - firsts
        return pl.pallas_call(
            functools.partial(kernel, n_sp, heads, head_dim),
            out_shape=pltpu.VMEM(latents.shape, bf16),
            in_specs=[any_spec, pl.BlockSpec(memory_space=pltpu.SMEM), pl.BlockSpec(memory_space=pltpu.VMEM)] + [any_spec] * 4,
            out_specs=pl.BlockSpec(memory_space=pltpu.VMEM),
            scratch_shapes=[
                pltpu.VMEM((rests, width, TILE), bf16), pltpu.VMEM((firsts, width, TILE), bf16),
                pltpu.VMEM((width, width), bf16),
                pltpu.VMEM((width, hidden), bf16), pltpu.VMEM((hidden, width), bf16),
                pltpu.VMEM((2, 2, n_sp // 2, rows // n_sp, width), bf16), pltpu.VMEM((2, half, 2 * width), bf16),
                pltpu.VMEM((width, rows), bf16),
                pltpu.VMEM((half, width), bf16), pltpu.VMEM((half, width), bf16),
                pltpu.VMEM((2, half, width), bf16),
                pltpu.VMEM((half, hidden), bf16), pltpu.VMEM((steps, rows // SUB, SUB, width), bf16),
                pltpu.VMEM((videos, rows // n_sp // SUB, n_sp * frames * SUB, width), bf16), pltpu.VMEM((half, half), f32),
                dma((3,)), dma((rests,)), dma((firsts,)), dma((2, 2)), dma((steps,)), dma((videos,)), dma,
            ],
            compiler_params=pltpu.CompilerParams(collective_id=0, has_side_effects=True, vmem_limit_bytes=62_000_000),
            cost_estimate=pl.CostEstimate(
                flops=2 * 2 * tokens * width * (4 * width + 2 * hidden), bytes_accessed=70_000_000, transcendentals=0),
            name="dit",
        )(latents.reshape(videos, frames, n_sp // 2, 2, rows // n_sp, width), valid_len, norm_w, w_qkv, w_out.reshape(2, width, width), w_up, w_down)

    return jax.shard_map(local_step, mesh=mesh, in_specs=(act_spec, P('data'), P(), P(), P(), P(), P()), out_specs=act_spec, check_vma=False)
```

```python
import functools
import math

import jax
import jax.numpy as jnp
from jax import lax
from jax.experimental import pallas as pl
from jax.experimental.pallas import tpu as pltpu
from jax.sharding import PartitionSpec as P

LN_EPS = 1e-6
MASKED = -1e30
OPEN = 3e38
LANES = 128
TILE = 256
SUB = 8
PACK = 16
f32, bf16 = jnp.float32, jnp.bfloat16
MESH = pl.DeviceIdType.MESH


def layer_norm(tokens, gain, shift):
    values = tokens.astype(f32)
    inv_width = 1.0 / values.shape[-1]
    centered = values - jnp.sum(values, -1, keepdims=True) * inv_width
    variance = jnp.sum(centered * centered, -1, keepdims=True) * inv_width
    return (centered * lax.rsqrt(variance + LN_EPS) * gain + shift).astype(bf16)


def project(a, b):
    return jnp.dot(a, b, preferred_element_type=f32).astype(bf16)


def residual(base, delta):
    return (base.astype(f32) + delta.astype(f32)).astype(bf16)


def gelu(u):
    x = u.astype(f32)
    c = math.sqrt(2.0 / math.pi)
    half = 0.5 * x
    return (half + half * jnp.tanh(x * (x * x * (c * 0.044715) + c))).astype(bf16)


def head_windows(heads, head_dim):
    out = []
    for h in range(heads):
        lo = h * head_dim
        base = lo // LANES * LANES
        out.append((lo, base, LANES if lo + head_dim <= base + LANES else 2 * LANES))
    return out


def column_tiles(wins, h, parts, width):
    _, base, w = wins[h]
    spans = [(p * width + base, p * width + base + w - 1) for p in parts]
    return list(dict.fromkeys(t for lo, hi in spans for t in range(lo // TILE, hi // TILE + 1)))


def columns(t, width):
    return slice(t * TILE, min((t + 1) * TILE, 3 * width))


def attend(nb, w_of, qk, vt, a_ref, heads, head_dim, place, mine, key_halves, made, look, lead, cap_ref):
    _, half, width = nb.shape
    scale = head_dim ** -0.5 * math.log2(math.e)
    wins = head_windows(heads, head_dim)
    made = set(made)

    def pieces(h, parts):
        return [(t, r) for p in parts for t in column_tiles(wins, h, (p,), width) for r in ((mine,) if p == 0 else key_halves)]

    def make(t, r):
        if (t, r) not in made:
            made.add((t, r))
            project_piece(nb, w_of(t), qk, vt, t, place(r))

    def keys(cols):
        return jnp.concatenate([qk[place(r), :, cols] for r in key_halves], axis=0)

    def scores(h):
        for u in pieces(h, (0, 1)):
            make(*u)
        lo, base, w_ = wins[h]
        lane = lax.broadcasted_iota(jnp.int32, (1, w_), 1) + base
        own = jnp.where((lane >= lo) & (lane < lo + head_dim), 1.0, 0.0).astype(bf16)
        q = qk[place(mine), :, base:base + w_] * own
        k = keys(slice(width + base, width + base + w_))
        return lax.dot_general(k, q, (((1,), (1,)), ((), ())), preferred_element_type=f32)

    due = []
    for h in range(heads):
        for p, step in ((0, h - look), (1, h - look), (2, h)):
            due += [(max(step, -1), u) for u in pieces(h, (p,))]
    ready = {h: scores(h) for h in range(look)}
    done, parts = 0, []
    for h in range(heads):
        for step, u in sorted(due, key=lambda d: d[0]):
            if step <= h + lead:
                make(*u)
        if h + look < heads:
            ready[h + look] = scores(h + look)
        s = ready.pop(h)
        if cap_ref is not None:
            s = jnp.minimum(s, cap_ref[...])
        e = jnp.exp2((s - jnp.max(s, 0, keepdims=True)) * scale)
        p = (e * (1.0 / jnp.sum(e, 0, keepdims=True))).astype(bf16)
        lo = h * head_dim
        r0, r1 = lo // PACK * PACK, pl.cdiv(lo + head_dim, PACK) * PACK
        v = jnp.concatenate([vt[place(r), r0:r1, :] for r in key_halves], axis=1)
        o = jnp.dot(v, p, preferred_element_type=f32)
        parts.append((lo, o[lo - r0:lo - r0 + head_dim, :]))
        while (done + 1) * LANES <= lo + head_dim:
            g0, g1 = done * LANES, (done + 1) * LANES
            rows = [x[max(g0 - l, 0):min(g1 - l, head_dim), :] for l, x in parts if l < g1]
            a_ref[:, g0:g1] = jnp.concatenate(rows, axis=0).astype(bf16).T
            parts = [(l, x) for l, x in parts if l + head_dim > g1]
            done += 1


def project_piece(nb, w, qk, vt, t, r):
    half, width = nb.shape[1:]
    piece = project(nb[r], w)
    cols = columns(t, width)
    if cols.start < 2 * width:
        qk[r, :, cols] = piece
    else:
        vt[r, cols.start - 2 * width:cols.stop - 2 * width, :] = piece.T


def kernel(n_sp, heads, head_dim, x_hbm, len_ref, norm_ref, wqkv_hbm, wout_hbm, wup_hbm, wdown_hbm, y_ref,
           wrest, wfirst, wout, wup, wdown, xb, qk, vt, ab, hb, n1, ub, zb, rb, cap,
           w_sem, rest_sem, first_sem, x_sem, send_sem, recv_sem, y_sem):
    videos, frames, pairs, _, per_dev, width = x_hbm.shape
    rows = pairs * 2 * per_dev
    steps = videos * frames
    half = rows // 2
    groups = per_dev // SUB
    chunks = groups // 2
    me = lax.axis_index("sp")
    peers = n_sp - 1

    barrier = pltpu.get_barrier_semaphore()

    @pl.loop(1, n_sp)
    def _(k):
        pl.semaphore_signal(barrier, inc=1, device_id={"sp": lax.rem(me + k, n_sp)}, device_id_type=MESH)

    weights = ((wout_hbm, wout), (wup_hbm, wup), (wdown_hbm, wdown))

    def load(i, layer):
        return pltpu.make_async_copy(weights[i][0].at[layer], weights[i][1], w_sem.at[i])

    def load_x(s, m):
        return pltpu.make_async_copy(
            x_hbm.at[s // frames, s % frames, :, m], xb.at[s % 2, m], x_sem.at[s % 2, m])

    tiles = pl.cdiv(3 * width, TILE)
    first = column_tiles(head_windows(heads, head_dim), 0, (0, 1, 2), width)
    rest = [t for t in range(tiles) if t not in first]
    extra = [t for t in range(width // TILE) if t not in first]

    def load_tile(t, layer):
        cols = columns(t, width)
        home, sem = (wfirst.at[first.index(t)], first_sem) if t in first else (wrest.at[rest.index(t)], rest_sem)
        size = cols.stop - cols.start
        return pltpu.make_async_copy(
            wqkv_hbm.at[layer, :, pl.ds(cols.start, size)], home.at[:, pl.ds(0, size)],
            sem.at[(first if t in first else rest).index(t)])

    def w_of(t):
        cols = columns(t, width)
        size = cols.stop - cols.start
        return wfirst[first.index(t)] if t in first else wrest[rest.index(t), :, :size]

    def norm_next(layer, s, m):
        norms = norm_ref[layer].astype(f32)
        n1[m] = layer_norm(xb[s % 2, m].reshape(half, width), norms[0:1], norms[1:2])

    def project_first(m):
        for t in first:
            project_piece(n1, w_of(t), qk, vt, t, m)

    for m in range(2):
        load_x(0, m).start()
    for t in first + rest:
        load_tile(t, 0).start()

    def frame_rows(s):
        return pl.ds(pl.multiple_of((me * frames + s % frames) * SUB, SUB), SUB)

    def send(s, m, pair):
        return pltpu.make_async_remote_copy(
            src_ref=zb.at[s, pl.ds((m * pairs + pair) * groups, groups)],
            dst_ref=rb.at[s // frames, :, frame_rows(s), :],
            send_sem=send_sem.at[s], recv_sem=recv_sem.at[s // frames],
            device_id={"sp": 2 * pair + m}, device_id_type=MESH)

    def result_rows(c, m):
        return pl.ds(pl.multiple_of(me * per_dev + (c % chunks * 2 + m) * SUB, SUB), SUB)

    def give(c, m, j):
        return pltpu.make_async_remote_copy(
            src_ref=zb.at[c, pl.ds((m * n_sp + j) * frames, frames)],
            dst_ref=y_ref.at[c // chunks, :, result_rows(c, m), :],
            send_sem=send_sem.at[c], recv_sem=y_sem, device_id={"sp": j}, device_id_type=MESH)

    def pair_at(i):
        turn = (i + 1) // 2 * (1 - 2 * (i % 2))
        return lax.rem(me // 2 + pairs // 2 + turn + pairs, pairs)

    def wait_sent(slot):
        sent = zb.at[slot, pl.ds(0, peers * groups)]
        pltpu.make_async_copy(sent, sent, send_sem.at[slot]).wait()

    for m in range(2):
        load_x(0, m).wait()
    for t in first:
        load_tile(t, 0).wait()
    for i in range(3):
        load(i, 0).start()
    for m in range(2):
        load_x(1, m).start()
    for m in range(2):
        norm_next(0, 0, m)
        project_first(m)
    for t in rest:
        load_tile(t, 0).wait()

    @pl.loop(0, 4 * steps)
    def _(turn):
        s, m = turn // 2, turn % 2
        spatial = s < steps
        temporal = s >= steps
        layer = s // steps
        slot = s % steps
        xs = xb.at[s % 2]
        attention = functools.partial(attend, n1, w_of, qk, vt, ab, heads, head_dim)
        there = {(t, r) for t in first for r in range(2)}

        def out(m):
            hb[...] = residual(xs[m].reshape(half, width), project(ab[...], wout[...]))

        def norm():
            norms = norm_ref[layer].astype(f32)
            ab[...] = layer_norm(hb[...], norms[2:3], norms[3:4])

        def up():
            ub[...] = gelu(project(ab[...], wup[...]))

        def down(m):
            z = residual(hb[...], project(ub[...], wdown[...]))
            zb[slot, m * (half // SUB):(m + 1) * (half // SUB)] = z.reshape(half // SUB, SUB, width)

        def second():
            @pl.when(s == steps - 1)
            def _():
                for t in rest:
                    load_tile(t, 1).start()
                for t in first:
                    load_tile(t, 1).wait()

            @pl.when(s + 1 < steps)
            def _():
                for m in range(2):
                    load_x(s + 1, m).wait()

            @pl.when(jnp.logical_and(s + 1 >= steps, s + 1 < 2 * steps))
            def _():
                c = s + 1 - steps

                @pl.when(c % chunks == 0)
                def _():
                    v = c // chunks
                    got = rb.at[v, :, pl.ds(0, peers * frames * SUB), :]
                    pltpu.make_async_copy(got, got, recv_sem.at[v]).wait()
                    shift = SUB.bit_length() - 1
                    limit = len_ref[v]
                    for r in range(0, half, LANES):
                        ki = lax.broadcasted_iota(jnp.int32, (LANES, half), 0) + r
                        qi = lax.broadcasted_iota(jnp.int32, (LANES, half), 1)
                        kt = lax.shift_right_logical(ki, shift)
                        ok = ((qi & (SUB - 1)) == (ki & (SUB - 1))) & (kt <= lax.shift_right_logical(qi, shift)) & (kt < limit)
                        cap[r:r + LANES, :] = jnp.where(ok, OPEN, MASKED)

                for m in range(2):
                    xb[(s + 1) % 2, m] = rb[c // chunks, c % chunks * 2 + m].reshape(pairs, per_dev, width)

            after = jnp.minimum((s + 1) // steps, 1)
            norm_next(after, s + 1, 0)
            out(1)
            load(0, after).start()
            project_first(0)
            norm()
            up()
            load(1, after).start()
            norm_next(after, s + 1, 1)
            project_first(1)
            down(1)

        @pl.when(jnp.logical_and(spatial, m == 0))
        def _():
            attention(lambda r: r, 0, (0, 1), there, 3, 2, None)

        @pl.when(jnp.logical_and(spatial, m == 1))
        def _():
            attention(lambda r: r, 1, (0, 1), {(t, r) for t in range(tiles) for r in range(2)}, 5, 3, None)

        @pl.when(temporal)
        def _():
            attention(lambda r: m, 0, (0,), there, 3, 3, cap)

        @pl.when(m == 0)
        def _():
            for i in range(2):
                load(i, layer).wait()

            @pl.when(slot == 0)
            def _():
                load(2, layer).wait()

            @pl.when(temporal)
            def _():
                wait_sent(slot)

            out(0)
            for t in extra:
                project_piece(n1, w_of(t), qk, vt, t, 1)
            norm()
            up()
            down(0)

            @pl.when(s == 0)
            def _():
                pl.semaphore_wait(barrier, peers)

        @pl.when(m == 1)
        def _():
            second()

        @pl.when(spatial)
        def _():
            @pl.loop(0, pairs)
            def _(i):
                pair = pair_at(i)

                @pl.when(2 * pair + m != me)
                def _():
                    send(s, m, pair).start()

            @pl.when(m == me % 2)
            def _():
                for g in range(groups):
                    rb[s // frames, g, frame_rows(s), :] = zb[s, (m * pairs + me // 2) * groups + g]

        @pl.when(temporal)
        def _():
            @pl.loop(0, pairs - 1)
            def _(i):
                for core in range(2):
                    give(slot, m, 2 * pair_at(i) + core).start()
            give(slot, m, me + 1 - 2 * (me % 2)).start()
            for f in range(frames):
                y_ref[slot // chunks, f, result_rows(slot, m), :] = zb[slot, (m * n_sp + me) * frames + f]

        @pl.when(m == 1)
        def _():

            @pl.when(s == steps - 1)
            def _():
                for t in rest:
                    load_tile(t, 1).wait()
                load(2, 1).start()

            @pl.when(s == steps - 2)
            def _():
                for t in first:
                    load_tile(t, 1).start()

            @pl.when(s + 2 < steps)
            def _():
                for m in range(2):
                    load_x(s + 2, m).start()

    for i in range(2):
        load(i, 1).wait()
    for slot in range(steps):
        wait_sent(slot)
    got = y_ref.at[:, :, pl.ds(0, peers * per_dev), :]
    pltpu.make_async_copy(got, got, y_sem).wait()


def solution(mesh):
    act_spec = P('data', 'sp', None, None)
    n_sp = mesh.shape['sp']

    def local_step(latents, valid_len, norm_w, w_qkv, w_out, w_up, w_down):
        videos, frames, rows, width = latents.shape
        heads, head_dim = w_out.shape[1:3]
        hidden = w_up.shape[2]
        tokens = videos * frames * rows
        half = rows // 2
        any_spec = pl.BlockSpec(memory_space=pl.ANY)
        dma = pltpu.SemaphoreType.DMA
        steps = videos * frames
        firsts = len(column_tiles(head_windows(heads, head_dim), 0, (0, 1, 2), width))
        rests = pl.cdiv(3 * width, TILE) - firsts
        return pl.pallas_call(
            functools.partial(kernel, n_sp, heads, head_dim),
            out_shape=pltpu.VMEM(latents.shape, bf16),
            in_specs=[any_spec, pl.BlockSpec(memory_space=pltpu.SMEM), pl.BlockSpec(memory_space=pltpu.VMEM)] + [any_spec] * 4,
            out_specs=pl.BlockSpec(memory_space=pltpu.VMEM),
            scratch_shapes=[
                pltpu.VMEM((rests, width, TILE), bf16), pltpu.VMEM((firsts, width, TILE), bf16),
                pltpu.VMEM((width, width), bf16),
                pltpu.VMEM((width, hidden), bf16), pltpu.VMEM((hidden, width), bf16),
                pltpu.VMEM((2, 2, n_sp // 2, rows // n_sp, width), bf16), pltpu.VMEM((2, half, 2 * width), bf16),
                pltpu.VMEM((2, width, half), bf16),
                pltpu.VMEM((half, width), bf16), pltpu.VMEM((half, width), bf16),
                pltpu.VMEM((2, half, width), bf16),
                pltpu.VMEM((half, hidden), bf16), pltpu.VMEM((steps, rows // SUB, SUB, width), bf16),
                pltpu.VMEM((videos, rows // n_sp // SUB, n_sp * frames * SUB, width), bf16), pltpu.VMEM((half, half), f32),
                dma((3,)), dma((rests,)), dma((firsts,)), dma((2, 2)), dma((steps,)), dma((videos,)), dma,
            ],
            compiler_params=pltpu.CompilerParams(collective_id=0, has_side_effects=True, vmem_limit_bytes=62_000_000),
            cost_estimate=pl.CostEstimate(
                flops=2 * 2 * tokens * width * (4 * width + 2 * hidden), bytes_accessed=70_000_000, transcendentals=0),
            name="dit",
        )(latents.reshape(videos, frames, n_sp // 2, 2, rows // n_sp, width), valid_len, norm_w, w_qkv, w_out.reshape(2, width, width), w_up, w_down)

    return jax.shard_map(local_step, mesh=mesh, in_specs=(act_spec, P('data'), P(), P(), P(), P(), P()), out_specs=act_spec, check_vma=False)
```

```python
import functools
import math

import jax
import jax.numpy as jnp
from jax import lax
from jax.experimental import pallas as pl
from jax.experimental.pallas import tpu as pltpu
from jax.sharding import PartitionSpec as P

LN_EPS = 1e-6
MASKED = -1e30
OPEN = 3e38
LANES = 128
TILE = 256
SUB = 8
FILL = 4
PACK = 16
f32, bf16 = jnp.float32, jnp.bfloat16
MESH = pl.DeviceIdType.MESH


def layer_norm(tokens, gain, shift):
    values = tokens.astype(f32)
    inv_width = 1.0 / values.shape[-1]
    centered = values - jnp.sum(values, -1, keepdims=True) * inv_width
    variance = jnp.sum(centered * centered, -1, keepdims=True) * inv_width
    return (centered * lax.rsqrt(variance + LN_EPS) * gain + shift).astype(bf16)


def project(a, b):
    return jnp.dot(a, b, preferred_element_type=f32).astype(bf16)


def residual(base, delta):
    return (base.astype(f32) + delta.astype(f32)).astype(bf16)


def gelu(u):
    x = u.astype(f32)
    c = math.sqrt(2.0 / math.pi)
    half = 0.5 * x
    return (half + half * jnp.tanh(x * (x * x * (c * 0.044715) + c))).astype(bf16)


def head_windows(heads, head_dim):
    out = []
    for h in range(heads):
        lo = h * head_dim
        base = lo // LANES * LANES
        out.append((lo, base, LANES if lo + head_dim <= base + LANES else 2 * LANES))
    return out


def column_tiles(wins, h, parts, width):
    _, base, w = wins[h]
    spans = [(p * width + base, p * width + base + w - 1) for p in parts]
    return list(dict.fromkeys(t for lo, hi in spans for t in range(lo // TILE, hi // TILE + 1)))


def columns(t, width):
    return slice(t * TILE, min((t + 1) * TILE, 3 * width))


def attend(nb, w_of, qk, vt, a_ref, heads, head_dim, mine, key_halves, made, look, lead, cap_ref, fill=()):
    _, half, width = nb.shape
    scale = head_dim ** -0.5 * math.log2(math.e)
    wins = head_windows(heads, head_dim)
    made = set(made)
    key_rows = slice(key_halves[0] * half, (key_halves[-1] + 1) * half)

    def pieces(h, parts):
        return [(t, r) for p in parts for t in column_tiles(wins, h, (p,), width) for r in ((mine,) if p == 0 else key_halves)]

    def make(t, r):
        if (t, r) not in made:
            made.add((t, r))
            project_piece(nb, w_of(t), qk, vt, t, r)

    def keys(cols):
        return jnp.concatenate([qk[r, :, cols] for r in key_halves], axis=0)

    def scores(h):
        for u in pieces(h, (0, 1)):
            make(*u)
        lo, base, w_ = wins[h]
        lane = lax.broadcasted_iota(jnp.int32, (1, w_), 1) + base
        own = jnp.where((lane >= lo) & (lane < lo + head_dim), 1.0, 0.0).astype(bf16)
        q = qk[mine, :, base:base + w_] * own
        k = keys(slice(width + base, width + base + w_))
        return lax.dot_general(k, q, (((1,), (1,)), ((), ())), preferred_element_type=f32)

    due = []
    for h in range(heads):
        for p, step in ((0, h - look), (1, h - look), (2, h)):
            due += [(max(step, -1), u) for u in pieces(h, (p,))]
    ready = {h: scores(h) for h in range(look)}
    done, parts = 0, []
    for h in range(heads):
        for step, u in sorted(due, key=lambda d: d[0]):
            if step <= h + lead:
                make(*u)
        if h + look < heads:
            ready[h + look] = scores(h + look)
        s = ready.pop(h)
        if cap_ref is not None:
            s = jnp.minimum(s, cap_ref[...])
        e = jnp.exp2((s - jnp.max(s, 0, keepdims=True)) * scale)
        p = (e * (1.0 / jnp.sum(e, 0, keepdims=True))).astype(bf16)
        if h >= heads - FILL:
            for f in fill[:pl.cdiv(len(fill), heads - h)]:
                f()
                fill = fill[1:]
        lo = h * head_dim
        r0, r1 = lo // PACK * PACK, pl.cdiv(lo + head_dim, PACK) * PACK
        o = jnp.dot(vt[r0:r1, key_rows], p, preferred_element_type=f32)
        parts.append((lo, o[lo - r0:lo - r0 + head_dim, :]))
        while (done + 1) * LANES <= lo + head_dim:
            g0, g1 = done * LANES, (done + 1) * LANES
            rows = [x[max(g0 - l, 0):min(g1 - l, head_dim), :] for l, x in parts if l < g1]
            a_ref[:, g0:g1] = jnp.concatenate(rows, axis=0).astype(bf16).T
            parts = [(l, x) for l, x in parts if l + head_dim > g1]
            done += 1


def project_piece(nb, w, qk, vt, t, r):
    half, width = nb.shape[1:]
    piece = project(nb[r], w)
    cols = columns(t, width)
    if cols.start < 2 * width:
        qk[r, :, cols] = piece
    else:
        vt[cols.start - 2 * width:cols.stop - 2 * width, r * half:(r + 1) * half] = piece.T


def kernel(n_sp, heads, head_dim, x_hbm, len_ref, norm_ref, wqkv_hbm, wout_hbm, wup_hbm, wdown_hbm, y_ref,
           wrest, wfirst, wout, wup, wdown, xb, qk, vt, ab, hb, n1, acc, ub, zb, rb, cap,
           w_sem, rest_sem, first_sem, x_sem, send_sem, recv_sem, y_sem):
    videos, frames, pairs, _, per_dev, width = x_hbm.shape
    rows = pairs * 2 * per_dev
    steps = videos * frames
    half = rows // 2
    groups = per_dev // SUB
    chunks = groups // 2
    me = lax.axis_index("sp")
    peers = n_sp - 1

    barrier = pltpu.get_barrier_semaphore()

    @pl.loop(1, n_sp)
    def _(k):
        pl.semaphore_signal(barrier, inc=1, device_id={"sp": lax.rem(me + k, n_sp)}, device_id_type=MESH)

    weights = ((wout_hbm, wout), (wup_hbm, wup), (wdown_hbm, wdown))

    def load(i, layer):
        return pltpu.make_async_copy(weights[i][0].at[layer], weights[i][1], w_sem.at[i])

    def load_x(s, m):
        return pltpu.make_async_copy(
            x_hbm.at[s // frames, s % frames, :, m], xb.at[s % 2, m], x_sem.at[s % 2, m])

    tiles = pl.cdiv(3 * width, TILE)
    first = column_tiles(head_windows(heads, head_dim), 0, (0, 1, 2), width)
    rest = [t for t in range(tiles) if t not in first]
    extra = [t for t in range(width // TILE) if t not in first]

    def load_tile(t, layer):
        cols = columns(t, width)
        home, sem = (wfirst.at[first.index(t)], first_sem) if t in first else (wrest.at[rest.index(t)], rest_sem)
        size = cols.stop - cols.start
        return pltpu.make_async_copy(
            wqkv_hbm.at[layer, :, pl.ds(cols.start, size)], home.at[:, pl.ds(0, size)],
            sem.at[(first if t in first else rest).index(t)])

    def w_of(t):
        cols = columns(t, width)
        size = cols.stop - cols.start
        return wfirst[first.index(t)] if t in first else wrest[rest.index(t), :, :size]

    def norm_next(layer, s, m):
        norms = norm_ref[layer].astype(f32)
        n1[m] = layer_norm(xb[s % 2, m].reshape(half, width), norms[0:1], norms[1:2])

    def project_first(m):
        for t in first:
            project_piece(n1, w_of(t), qk, vt, t, m)

    for m in range(2):
        load_x(0, m).start()
    for t in first + rest:
        load_tile(t, 0).start()
    load(0, 0).start()

    def frame_rows(s):
        return pl.ds(pl.multiple_of((me * frames + s % frames) * SUB, SUB), SUB)

    def send(s, m, pair):
        return pltpu.make_async_remote_copy(
            src_ref=zb.at[s, pl.ds((m * pairs + pair) * groups, groups)],
            dst_ref=rb.at[s // frames, :, frame_rows(s), :],
            send_sem=send_sem.at[s], recv_sem=recv_sem.at[s // frames],
            device_id={"sp": 2 * pair + m}, device_id_type=MESH)

    def result_rows(c, m):
        return pl.ds(pl.multiple_of(me * per_dev + (c % chunks * 2 + m) * SUB, SUB), SUB)

    def give(c, m, j):
        return pltpu.make_async_remote_copy(
            src_ref=zb.at[c, pl.ds((m * n_sp + j) * frames, frames)],
            dst_ref=y_ref.at[c // chunks, :, result_rows(c, m), :],
            send_sem=send_sem.at[c], recv_sem=y_sem, device_id={"sp": j}, device_id_type=MESH)

    def pair_at(i):
        turn = (i + 1) // 2 * (1 - 2 * (i % 2))
        return lax.rem(me // 2 + pairs // 2 + turn + pairs, pairs)

    def wait_sent(slot):
        sent = zb.at[slot, pl.ds(0, peers * groups)]
        pltpu.make_async_copy(sent, sent, send_sem.at[slot]).wait()

    for m in range(2):
        load_x(0, m).wait()
    for t in first:
        load_tile(t, 0).wait()
    for i in range(1, 3):
        load(i, 0).start()
    for m in range(2):
        load_x(1, m).start()
    for m in range(2):
        norm_next(0, 0, m)
        project_first(m)
    for t in rest:
        load_tile(t, 0).wait()

    @pl.loop(0, 2 * steps)
    def _(s):
        spatial = s < steps
        temporal = s >= steps
        layer = s // steps
        slot = s % steps
        xs = xb.at[s % 2]
        attention = functools.partial(attend, n1, w_of, qk, vt, ab, heads, head_dim)
        there = {(t, r) for t in first for r in range(2)}

        def out(m):
            hb[...] = residual(xs[m].reshape(half, width), project(ab[...], wout[...]))

        depth = width * 2 // 3 // TILE * TILE

        def out_start(j):
            cols = slice(j, min(j + TILE, width))
            acc[:, cols] = jnp.dot(ab[:, :depth], wout[:depth, cols], preferred_element_type=f32)

        def out_rest(m):
            late = jnp.dot(ab[:, depth:], wout[depth:, :], preferred_element_type=f32)
            hb[...] = residual(xs[m].reshape(half, width), (acc[...] + late).astype(bf16))

        early = [functools.partial(out_start, j) for j in range(0, width, TILE)]

        def norm():
            norms = norm_ref[layer].astype(f32)
            ab[...] = layer_norm(hb[...], norms[2:3], norms[3:4])

        def up():
            ub[...] = gelu(project(ab[...], wup[...]))

        def down(m):
            z = residual(hb[...], project(ub[...], wdown[...]))
            zb[slot, m * (half // SUB):(m + 1) * (half // SUB)] = z.reshape(half // SUB, SUB, width)

        def deliver(m):
            @pl.when(spatial)
            def _():
                for i in range(pairs - 1):
                    send(s, m, pair_at(i)).start()

                @pl.when(m != me % 2)
                def _():
                    send(s, m, me // 2).start()

                @pl.when(m == me % 2)
                def _():
                    for g in range(groups):
                        rb[s // frames, g, frame_rows(s), :] = zb[s, (m * pairs + me // 2) * groups + g]

            @pl.when(temporal)
            def _():
                @pl.loop(0, pairs - 1)
                def _(i):
                    for core in range(2):
                        give(slot, m, 2 * pair_at(i) + core).start()
                give(slot, m, me + 1 - 2 * (me % 2)).start()
                for f in range(frames):
                    y_ref[slot // chunks, f, result_rows(slot, m), :] = zb[slot, (m * n_sp + me) * frames + f]

        load(0, layer).wait()

        @pl.when(spatial)
        def _():
            attention(0, (0, 1), there, 3, 2, None, early)

        @pl.when(temporal)
        def _():
            attention(0, (0,), there, 3, 3, cap, early)

        load(1, layer).wait()

        @pl.when(slot == 0)
        def _():
            load(2, layer).wait()

        @pl.when(temporal)
        def _():
            wait_sent(slot)

        out_rest(0)
        for t in extra:
            project_piece(n1, w_of(t), qk, vt, t, 1)
        norm()
        up()
        down(0)

        @pl.when(s == 0)
        def _():
            pl.semaphore_wait(barrier, peers)

        deliver(0)

        @pl.when(spatial)
        def _():
            attention(1, (0, 1), {(t, r) for t in range(tiles) for r in range(2)}, 5, 3, None)

        @pl.when(temporal)
        def _():
            attention(1, (1,), there | {(t, 1) for t in extra}, 4, 3, cap)

        @pl.when(s == steps - 1)
        def _():
            for t in rest:
                load_tile(t, 1).start()
            for t in first:
                load_tile(t, 1).wait()

        @pl.when(s + 1 < steps)
        def _():
            for m in range(2):
                load_x(s + 1, m).wait()

        @pl.when(jnp.logical_and(s + 1 >= steps, s + 1 < 2 * steps))
        def _():
            c = s + 1 - steps

            @pl.when(c % chunks == 0)
            def _():
                v = c // chunks
                got = rb.at[v, :, pl.ds(0, peers * frames * SUB), :]
                pltpu.make_async_copy(got, got, recv_sem.at[v]).wait()
                shift = SUB.bit_length() - 1
                limit = len_ref[v]
                for r in range(0, half, LANES):
                    ki = lax.broadcasted_iota(jnp.int32, (LANES, half), 0) + r
                    qi = lax.broadcasted_iota(jnp.int32, (LANES, half), 1)
                    kt = lax.shift_right_logical(ki, shift)
                    ok = ((qi & (SUB - 1)) == (ki & (SUB - 1))) & (kt <= lax.shift_right_logical(qi, shift)) & (kt < limit)
                    cap[r:r + LANES, :] = jnp.where(ok, OPEN, MASKED)

            for m in range(2):
                xb[(s + 1) % 2, m] = rb[c // chunks, c % chunks * 2 + m].reshape(pairs, per_dev, width)

        after = jnp.minimum((s + 1) // steps, 1)
        norm_next(after, s + 1, 0)
        out(1)
        load(0, after).start()
        project_first(0)
        norm()
        up()
        load(1, after).start()
        norm_next(after, s + 1, 1)
        project_first(1)
        down(1)
        deliver(1)

        @pl.when(s == steps - 1)
        def _():
            for t in rest:
                load_tile(t, 1).wait()
            load(2, 1).start()

        @pl.when(s == steps - 2)
        def _():
            for t in first:
                load_tile(t, 1).start()

        @pl.when(s + 2 < steps)
        def _():
            for m in range(2):
                load_x(s + 2, m).start()

    for i in range(2):
        load(i, 1).wait()
    for slot in range(steps):
        wait_sent(slot)
    got = y_ref.at[:, :, pl.ds(0, peers * per_dev), :]
    pltpu.make_async_copy(got, got, y_sem).wait()


def solution(mesh):
    act_spec = P('data', 'sp', None, None)
    n_sp = mesh.shape['sp']

    def local_step(latents, valid_len, norm_w, w_qkv, w_out, w_up, w_down):
        videos, frames, rows, width = latents.shape
        heads, head_dim = w_out.shape[1:3]
        hidden = w_up.shape[2]
        tokens = videos * frames * rows
        half = rows // 2
        any_spec = pl.BlockSpec(memory_space=pl.ANY)
        dma = pltpu.SemaphoreType.DMA
        steps = videos * frames
        firsts = len(column_tiles(head_windows(heads, head_dim), 0, (0, 1, 2), width))
        rests = pl.cdiv(3 * width, TILE) - firsts
        return pl.pallas_call(
            functools.partial(kernel, n_sp, heads, head_dim),
            out_shape=pltpu.VMEM(latents.shape, bf16),
            in_specs=[any_spec, pl.BlockSpec(memory_space=pltpu.SMEM), pl.BlockSpec(memory_space=pltpu.VMEM)] + [any_spec] * 4,
            out_specs=pl.BlockSpec(memory_space=pltpu.VMEM),
            scratch_shapes=[
                pltpu.VMEM((rests, width, TILE), bf16), pltpu.VMEM((firsts, width, TILE), bf16),
                pltpu.VMEM((width, width), bf16),
                pltpu.VMEM((width, hidden), bf16), pltpu.VMEM((hidden, width), bf16),
                pltpu.VMEM((2, 2, n_sp // 2, rows // n_sp, width), bf16), pltpu.VMEM((2, half, 2 * width), bf16),
                pltpu.VMEM((width, rows), bf16),
                pltpu.VMEM((half, width), bf16), pltpu.VMEM((half, width), bf16),
                pltpu.VMEM((2, half, width), bf16),
                pltpu.VMEM((half, width), f32), pltpu.VMEM((half, hidden), bf16), pltpu.VMEM((steps, rows // SUB, SUB, width), bf16),
                pltpu.VMEM((videos, rows // n_sp // SUB, n_sp * frames * SUB, width), bf16), pltpu.VMEM((half, half), f32),
                dma((3,)), dma((rests,)), dma((firsts,)), dma((2, 2)), dma((steps,)), dma((videos,)), dma,
            ],
            compiler_params=pltpu.CompilerParams(collective_id=0, has_side_effects=True, vmem_limit_bytes=62_000_000),
            cost_estimate=pl.CostEstimate(
                flops=2 * 2 * tokens * width * (4 * width + 2 * hidden), bytes_accessed=70_000_000, transcendentals=0),
            name="dit",
        )(latents.reshape(videos, frames, n_sp // 2, 2, rows // n_sp, width), valid_len, norm_w, w_qkv, w_out.reshape(2, width, width), w_up, w_down)

    return jax.shard_map(local_step, mesh=mesh, in_specs=(act_spec, P('data'), P(), P(), P(), P(), P()), out_specs=act_spec, check_vma=False)
```

```python
import functools
import math

import jax
import jax.numpy as jnp
from jax import lax
from jax.experimental import pallas as pl
from jax.experimental.pallas import tpu as pltpu
from jax.sharding import PartitionSpec as P

LN_EPS = 1e-6
MASKED = -1e30
OPEN = math.inf
LANES = 128
TILE = 256
SUB = 8
FILL = 4
PACK = 16
f32, bf16 = jnp.float32, jnp.bfloat16
MESH = pl.DeviceIdType.MESH


def layer_norm(tokens, gain, shift):
    values = tokens.astype(f32)
    inv_width = 1.0 / values.shape[-1]
    centered = values - jnp.sum(values, -1, keepdims=True) * inv_width
    variance = jnp.sum(centered * centered, -1, keepdims=True) * inv_width
    return (centered * lax.rsqrt(variance + LN_EPS) * gain + shift).astype(bf16)


def project(a, b):
    return jnp.dot(a, b, preferred_element_type=f32).astype(bf16)


def residual(base, delta):
    return (base.astype(f32) + delta.astype(f32)).astype(bf16)


def gelu(u):
    x = u.astype(f32)
    c = math.sqrt(2.0 / math.pi)
    half = 0.5 * x
    return (half + half * jnp.tanh(x * (x * x * (c * 0.044715) + c))).astype(bf16)


def head_windows(heads, head_dim):
    out = []
    for h in range(heads):
        lo = h * head_dim
        base = lo // LANES * LANES
        out.append((lo, base, LANES if lo + head_dim <= base + LANES else 2 * LANES))
    return out


def column_tiles(wins, h, parts, width):
    _, base, w = wins[h]
    spans = [(p * width + base, p * width + base + w - 1) for p in parts]
    return list(dict.fromkeys(t for lo, hi in spans for t in range(lo // TILE, hi // TILE + 1)))


def columns(t, width):
    return slice(t * TILE, min((t + 1) * TILE, 3 * width))


def attend(nb, w_of, qk, vt, a_ref, heads, head_dim, mine, key_halves, made, look, lead, cap_ref, fill=()):
    _, half, width = nb.shape
    scale = head_dim ** -0.5 * math.log2(math.e)
    wins = head_windows(heads, head_dim)
    made = set(made)
    key_rows = slice(key_halves[0] * half, (key_halves[-1] + 1) * half)

    def pieces(h, parts):
        return [(t, r) for p in parts for t in column_tiles(wins, h, (p,), width) for r in ((mine,) if p == 0 else key_halves)]

    def make(t, r):
        if (t, r) not in made:
            made.add((t, r))
            project_piece(nb, w_of(t), qk, vt, t, r)

    def keys(cols):
        return jnp.concatenate([qk[r, :, cols] for r in key_halves], axis=0)

    def scores(h):
        for u in pieces(h, (0, 1)):
            make(*u)
        lo, base, w_ = wins[h]
        lane = lax.broadcasted_iota(jnp.int32, (1, w_), 1) + base
        own = jnp.where((lane >= lo) & (lane < lo + head_dim), 1.0, 0.0).astype(bf16)
        q = qk[mine, :, base:base + w_] * own
        k = keys(slice(width + base, width + base + w_))
        return lax.dot_general(k, q, (((1,), (1,)), ((), ())), preferred_element_type=f32)

    due = []
    for h in range(heads):
        for p, step in ((0, h - look), (1, h - look), (2, h)):
            due += [(max(step, -1), u) for u in pieces(h, (p,))]
    ready = {h: scores(h) for h in range(look)}
    done, parts = 0, []
    for h in range(heads):
        for step, u in sorted(due, key=lambda d: d[0]):
            if step <= h + lead:
                make(*u)
        if h + look < heads:
            ready[h + look] = scores(h + look)
        s = ready.pop(h)
        if cap_ref is not None:
            s = jnp.minimum(s, cap_ref[...])
        e = jnp.exp2((s - jnp.max(s, 0, keepdims=True)) * scale)
        p = (e * (1.0 / jnp.sum(e, 0, keepdims=True))).astype(bf16)
        if h >= heads - FILL:
            for f in fill[:pl.cdiv(len(fill), heads - h)]:
                f()
                fill = fill[1:]
        lo = h * head_dim
        r0, r1 = lo // PACK * PACK, pl.cdiv(lo + head_dim, PACK) * PACK
        o = jnp.dot(vt[r0:r1, key_rows], p, preferred_element_type=f32)
        parts.append((lo, o[lo - r0:lo - r0 + head_dim, :]))
        while (done + 1) * LANES <= lo + head_dim:
            g0, g1 = done * LANES, (done + 1) * LANES
            rows = [x[max(g0 - l, 0):min(g1 - l, head_dim), :] for l, x in parts if l < g1]
            a_ref[:, g0:g1] = jnp.concatenate(rows, axis=0).astype(bf16).T
            parts = [(l, x) for l, x in parts if l + head_dim > g1]
            done += 1


def project_piece(nb, w, qk, vt, t, r):
    half, width = nb.shape[1:]
    piece = project(nb[r], w)
    cols = columns(t, width)
    if cols.start < 2 * width:
        qk[r, :, cols] = piece
    else:
        vt[cols.start - 2 * width:cols.stop - 2 * width, r * half:(r + 1) * half] = piece.T


def kernel(n_sp, heads, head_dim, x_hbm, len_ref, norm_ref, wqkv_hbm, wout_hbm, wup_hbm, wdown_hbm, y_ref,
           wrest, wfirst, wout, wup, wdown, xb, qk, vt, ab, hb, n1, acc, ub, zb, rb, cap,
           w_sem, rest_sem, first_sem, x_sem, send_sem, recv_sem, y_sem):
    videos, frames, pairs, _, per_dev, width = x_hbm.shape
    rows = pairs * 2 * per_dev
    steps = videos * frames
    half = rows // 2
    groups = per_dev // SUB
    chunks = groups // 2
    me = lax.axis_index("sp")
    peers = n_sp - 1

    barrier = pltpu.get_barrier_semaphore()

    @pl.loop(1, n_sp)
    def _(k):
        pl.semaphore_signal(barrier, inc=1, device_id={"sp": lax.rem(me + k, n_sp)}, device_id_type=MESH)

    weights = ((wout_hbm, wout), (wup_hbm, wup), (wdown_hbm, wdown))

    def load(i, layer):
        return pltpu.make_async_copy(weights[i][0].at[layer], weights[i][1], w_sem.at[i])

    def load_x(s, m):
        return pltpu.make_async_copy(
            x_hbm.at[s // frames, s % frames, :, m], xb.at[s % 2, m], x_sem.at[s % 2, m])

    tiles = pl.cdiv(3 * width, TILE)
    first = column_tiles(head_windows(heads, head_dim), 0, (0, 1, 2), width)
    rest = [t for t in range(tiles) if t not in first]
    extra = [t for t in range(width // TILE) if t not in first]

    def load_tile(t, layer):
        cols = columns(t, width)
        home, sem = (wfirst.at[first.index(t)], first_sem) if t in first else (wrest.at[rest.index(t)], rest_sem)
        size = cols.stop - cols.start
        return pltpu.make_async_copy(
            wqkv_hbm.at[layer, :, pl.ds(cols.start, size)], home.at[:, pl.ds(0, size)],
            sem.at[(first if t in first else rest).index(t)])

    def w_of(t):
        cols = columns(t, width)
        size = cols.stop - cols.start
        return wfirst[first.index(t)] if t in first else wrest[rest.index(t), :, :size]

    def norm_next(layer, s, m):
        norms = norm_ref[layer].astype(f32)
        n1[m] = layer_norm(xb[s % 2, m].reshape(half, width), norms[0:1], norms[1:2])

    def project_first(m):
        for t in first:
            project_piece(n1, w_of(t), qk, vt, t, m)

    for m in range(2):
        load_x(0, m).start()
    for t in first + rest:
        load_tile(t, 0).start()
    load(0, 0).start()

    def frame_rows(s):
        return pl.ds(pl.multiple_of((me * frames + s % frames) * SUB, SUB), SUB)

    def send(s, m, pair):
        return pltpu.make_async_remote_copy(
            src_ref=zb.at[s, pl.ds((m * pairs + pair) * groups, groups)],
            dst_ref=rb.at[s // frames, :, frame_rows(s), :],
            send_sem=send_sem.at[s], recv_sem=recv_sem.at[s // frames],
            device_id={"sp": 2 * pair + m}, device_id_type=MESH)

    def result_rows(c, m):
        return pl.ds(pl.multiple_of(me * per_dev + (c % chunks * 2 + m) * SUB, SUB), SUB)

    def give(c, m, j):
        return pltpu.make_async_remote_copy(
            src_ref=zb.at[c, pl.ds((m * n_sp + j) * frames, frames)],
            dst_ref=y_ref.at[c // chunks, :, result_rows(c, m), :],
            send_sem=send_sem.at[c], recv_sem=y_sem, device_id={"sp": j}, device_id_type=MESH)

    def pair_at(i):
        turn = (i + 1) // 2 * (1 - 2 * (i % 2))
        return lax.rem(me // 2 + pairs // 2 + turn + pairs, pairs)

    def wait_sent(slot):
        sent = zb.at[slot, pl.ds(0, peers * groups)]
        pltpu.make_async_copy(sent, sent, send_sem.at[slot]).wait()

    for m in range(2):
        load_x(0, m).wait()
    for t in first:
        load_tile(t, 0).wait()
    for i in range(1, 3):
        load(i, 0).start()
    for m in range(2):
        load_x(1, m).start()
    for m in range(2):
        norm_next(0, 0, m)
        project_first(m)
    for t in rest:
        load_tile(t, 0).wait()

    @pl.loop(0, 2 * steps)
    def _(s):
        spatial = s < steps
        temporal = s >= steps
        layer = s // steps
        slot = s % steps
        xs = xb.at[s % 2]
        attention = functools.partial(attend, n1, w_of, qk, vt, ab, heads, head_dim)
        there = {(t, r) for t in first for r in range(2)}

        def out(m):
            hb[...] = residual(xs[m].reshape(half, width), project(ab[...], wout[...]))

        depth = width * 2 // 3 // TILE * TILE

        def out_start(j):
            cols = slice(j, min(j + TILE, width))
            acc[:, cols] = jnp.dot(ab[:, :depth], wout[:depth, cols], preferred_element_type=f32)

        def out_rest(m):
            late = jnp.dot(ab[:, depth:], wout[depth:, :], preferred_element_type=f32)
            hb[...] = residual(xs[m].reshape(half, width), (acc[...] + late).astype(bf16))

        early = [functools.partial(out_start, j) for j in range(0, width, TILE)]

        def norm():
            norms = norm_ref[layer].astype(f32)
            ab[...] = layer_norm(hb[...], norms[2:3], norms[3:4])

        def up():
            ub[...] = gelu(project(ab[...], wup[...]))

        def down(m):
            z = residual(hb[...], project(ub[...], wdown[...]))
            zb[slot, m * (half // SUB):(m + 1) * (half // SUB)] = z.reshape(half // SUB, SUB, width)

        def deliver(m):
            @pl.when(spatial)
            def _():
                for i in range(pairs - 1):
                    send(s, m, pair_at(i)).start()

                @pl.when(m != me % 2)
                def _():
                    send(s, m, me // 2).start()

                @pl.when(m == me % 2)
                def _():
                    for g in range(groups):
                        rb[s // frames, g, frame_rows(s), :] = zb[s, (m * pairs + me // 2) * groups + g]

            @pl.when(temporal)
            def _():
                @pl.loop(0, pairs - 1)
                def _(i):
                    for core in range(2):
                        give(slot, m, 2 * pair_at(i) + core).start()
                give(slot, m, me + 1 - 2 * (me % 2)).start()
                for f in range(frames):
                    y_ref[slot // chunks, f, result_rows(slot, m), :] = zb[slot, (m * n_sp + me) * frames + f]

        load(0, layer).wait()

        @pl.when(spatial)
        def _():
            attention(0, (0, 1), there, 3, 2, None, early)

        @pl.when(temporal)
        def _():
            attention(0, (0,), there, 3, 3, cap, early)

        load(1, layer).wait()

        @pl.when(slot == 0)
        def _():
            load(2, layer).wait()

        @pl.when(temporal)
        def _():
            wait_sent(slot)

        out_rest(0)
        for t in extra:
            project_piece(n1, w_of(t), qk, vt, t, 1)
        norm()
        up()
        down(0)

        @pl.when(s == 0)
        def _():
            pl.semaphore_wait(barrier, peers)

        deliver(0)

        @pl.when(spatial)
        def _():
            attention(1, (0, 1), {(t, r) for t in range(tiles) for r in range(2)}, 5, 3, None)

        @pl.when(temporal)
        def _():
            attention(1, (1,), there | {(t, 1) for t in extra}, 4, 3, cap)

        @pl.when(s == steps - 1)
        def _():
            for t in rest:
                load_tile(t, 1).start()
            for t in first:
                load_tile(t, 1).wait()

        @pl.when(s + 1 < steps)
        def _():
            for m in range(2):
                load_x(s + 1, m).wait()

        @pl.when(jnp.logical_and(s + 1 >= steps, s + 1 < 2 * steps))
        def _():
            c = s + 1 - steps

            @pl.when(c % chunks == 0)
            def _():
                v = c // chunks
                got = rb.at[v, :, pl.ds(0, peers * frames * SUB), :]
                pltpu.make_async_copy(got, got, recv_sem.at[v]).wait()
                shift = SUB.bit_length() - 1
                limit = len_ref[v]
                for r in range(0, half, LANES):
                    ki = lax.broadcasted_iota(jnp.int32, (LANES, half), 0) + r
                    qi = lax.broadcasted_iota(jnp.int32, (LANES, half), 1)
                    kt = lax.shift_right_logical(ki, shift)
                    ok = ((qi & (SUB - 1)) == (ki & (SUB - 1))) & (kt <= lax.shift_right_logical(qi, shift)) & (kt < limit)
                    cap[r:r + LANES, :] = jnp.where(ok, OPEN, MASKED * head_dim ** 0.5)

            for m in range(2):
                xb[(s + 1) % 2, m] = rb[c // chunks, c % chunks * 2 + m].reshape(pairs, per_dev, width)

        after = jnp.minimum((s + 1) // steps, 1)
        norm_next(after, s + 1, 0)
        out(1)
        load(0, after).start()
        project_first(0)
        norm()
        up()
        load(1, after).start()
        norm_next(after, s + 1, 1)
        project_first(1)
        down(1)
        deliver(1)

        @pl.when(s == steps - 1)
        def _():
            for t in rest:
                load_tile(t, 1).wait()
            load(2, 1).start()

        @pl.when(s == steps - 2)
        def _():
            for t in first:
                load_tile(t, 1).start()

        @pl.when(s + 2 < steps)
        def _():
            for m in range(2):
                load_x(s + 2, m).start()

    for i in range(2):
        load(i, 1).wait()
    for slot in range(steps):
        wait_sent(slot)
    got = y_ref.at[:, :, pl.ds(0, peers * per_dev), :]
    pltpu.make_async_copy(got, got, y_sem).wait()


def solution(mesh):
    act_spec = P('data', 'sp', None, None)
    n_sp = mesh.shape['sp']

    def local_step(latents, valid_len, norm_w, w_qkv, w_out, w_up, w_down):
        videos, frames, rows, width = latents.shape
        heads, head_dim = w_out.shape[1:3]
        hidden = w_up.shape[2]
        tokens = videos * frames * rows
        half = rows // 2
        any_spec = pl.BlockSpec(memory_space=pl.ANY)
        dma = pltpu.SemaphoreType.DMA
        steps = videos * frames
        firsts = len(column_tiles(head_windows(heads, head_dim), 0, (0, 1, 2), width))
        rests = pl.cdiv(3 * width, TILE) - firsts
        return pl.pallas_call(
            functools.partial(kernel, n_sp, heads, head_dim),
            out_shape=pltpu.VMEM(latents.shape, bf16),
            in_specs=[any_spec, pl.BlockSpec(memory_space=pltpu.SMEM), pl.BlockSpec(memory_space=pltpu.VMEM)] + [any_spec] * 4,
            out_specs=pl.BlockSpec(memory_space=pltpu.VMEM),
            scratch_shapes=[
                pltpu.VMEM((rests, width, TILE), bf16), pltpu.VMEM((firsts, width, TILE), bf16),
                pltpu.VMEM((width, width), bf16),
                pltpu.VMEM((width, hidden), bf16), pltpu.VMEM((hidden, width), bf16),
                pltpu.VMEM((2, 2, n_sp // 2, rows // n_sp, width), bf16), pltpu.VMEM((2, half, 2 * width), bf16),
                pltpu.VMEM((width, rows), bf16),
                pltpu.VMEM((half, width), bf16), pltpu.VMEM((half, width), bf16),
                pltpu.VMEM((2, half, width), bf16),
                pltpu.VMEM((half, width), f32), pltpu.VMEM((half, hidden), bf16), pltpu.VMEM((steps, rows // SUB, SUB, width), bf16),
                pltpu.VMEM((videos, rows // n_sp // SUB, n_sp * frames * SUB, width), bf16), pltpu.VMEM((half, half), f32),
                dma((3,)), dma((rests,)), dma((firsts,)), dma((2, 2)), dma((steps,)), dma((videos,)), dma,
            ],
            compiler_params=pltpu.CompilerParams(collective_id=0, has_side_effects=True, vmem_limit_bytes=62_000_000),
            cost_estimate=pl.CostEstimate(
                flops=2 * 2 * tokens * width * (4 * width + 2 * hidden), bytes_accessed=70_000_000, transcendentals=0),
            name="dit",
        )(latents.reshape(videos, frames, n_sp // 2, 2, rows // n_sp, width), valid_len, norm_w, w_qkv, w_out.reshape(2, width, width), w_up, w_down)

    return jax.shard_map(local_step, mesh=mesh, in_specs=(act_spec, P('data'), P(), P(), P(), P(), P()), out_specs=act_spec, check_vma=False)
```
